32 devices in a mesh: gz: 8 (over z, x), gx: 4 (over y, core).
Axes of the slice: x: 2, y: 2, z: 4, core: 2. Of those that a mesh axis runs over, the one named last changes fastest.
Arguments:
- noisy_volume: float32 [32, 512, 512], P('gz', 'gx'), may hold values from -3 to 3, as said below
- tv_weight: float32 [32, 512, 512], P('gz', 'gx'), may hold values from 0.05 to 0.5
Outputs:
- denoised: float32 [32, 512, 512], P('gz', 'gx')
- gap_values: float32 [4], replicated
- step_values: float32 [4], replicated
The draws below stay inside these ranges and needn't reach their ends.
Inputs may be any that keep to these rules, and one draw needn't show every extreme that they name: `noisy_volume`: voxel intensities.
All inputs are finite; a program needn't handle non-finite values.
Results may differ from the reference program's by a relative error of at most 0.0001.
Values sent between devices are 32-bit elements; how exact they have to be, the bound alone decides.
No kernel may reach another device: no remote copies, remote signals or barrier semaphores. Data moves between devices by JAX's collectives and lax.ppermute only.
A program may use at most 64 MiB of HBM per device.

```python
import math
import jax
import jax.numpy as jnp

ITERS = 4
NZ = 32
NX = 512
NY = 512


def draw_noisy_volume(key, part):
    base = jax.random.fold_in(key, 11)
    key_rough = jax.random.fold_in(base, 0)
    position = jnp.arange(NZ, dtype=jnp.float32) / max(NZ - 1, 1)
    rough = jax.random.uniform(key_rough, (NZ, NX, NY), jnp.float32, minval=-1.0, maxval=1.0)
    planes_scale = (3.0 ** position)[:, None, None]
    volume = planes_scale * rough
    return volume.astype(jnp.float32)


def block_scale(own_key, extent, pieces, low, largest):
    gain = 1.0
    for dim, parts in pieces:
        steps = jax.random.uniform(jax.random.fold_in(jax.random.fold_in(own_key, 6), dim), (parts,), jnp.float32, low / len(pieces), largest / len(pieces))
        gain = gain * jnp.repeat(jnp.exp(steps), extent[dim] // parts).reshape((-1,) + (1,) * (len(extent) - 1 - dim))
    return gain


def setup_inputs(seed: int = 0) -> dict:
    keys = jax.random.split(jax.random.key(seed), 3)
    return {
        "noisy_volume": draw_noisy_volume(jax.random.fold_in(keys[2], 71), 0),
        "tv_weight": jnp.clip(jnp.exp(math.log(0.5) - 2.3025851 * jax.random.uniform(keys[1], (NZ, NX, NY), jnp.float32) ** block_scale(keys[1], (NZ, NX, NY), ((0, 8), (1, 4)), -0.2, 0.2)), 0.05, 0.5),
    }


primal_step = 0.28
dual_step = 0.28

def gradient(volume):
    along_z = jnp.concatenate([volume[1:] - volume[:-1], jnp.zeros_like(volume[:1])], axis=0)
    along_x = jnp.concatenate([volume[:, 1:] - volume[:, :-1], jnp.zeros_like(volume[:, :1])], axis=1)
    along_y = jnp.concatenate([volume[:, :, 1:] - volume[:, :, :-1], jnp.zeros_like(volume[:, :, :1])], axis=2)
    return (along_z, along_x, along_y)

def divergence(dual_field):
    dual_z, dual_x, dual_y = dual_field
    back_z = dual_z - jnp.concatenate([jnp.zeros_like(dual_z[:1]), dual_z[:-1]], axis=0)
    back_x = dual_x - jnp.concatenate([jnp.zeros_like(dual_x[:, :1]), dual_x[:, :-1]], axis=1)
    back_y = dual_y - jnp.concatenate([jnp.zeros_like(dual_y[:, :, :1]), dual_y[:, :, :-1]], axis=2)
    return back_z + back_x + back_y

def reference(noisy_volume, tv_weight):
    cell_count = noisy_volume.shape[0] * noisy_volume.shape[1] * noisy_volume.shape[2]
    primal = noisy_volume
    extrapolated = noisy_volume
    zeros_field = jnp.zeros_like(noisy_volume)
    dual_field = (zeros_field, zeros_field, zeros_field)
    gap_list = []
    step_list = []
    for iteration in range(ITERS):
        grad_extra = gradient(extrapolated)
        grad_primal = gradient(primal)
        proposed = tuple((dual_part + dual_step * grad_part for dual_part, grad_part in zip(dual_field, grad_extra)))
        magnitude = jnp.sqrt(proposed[0] * proposed[0] + proposed[1] * proposed[1] + proposed[2] * proposed[2])
        shrink = tv_weight / jnp.maximum(tv_weight, magnitude)
        dual_field = tuple((part * shrink for part in proposed))
        spread = divergence(dual_field)
        updated = (primal + primal_step * (spread + noisy_volume)) / (1.0 + primal_step)
        total_var = jnp.sqrt(grad_primal[0] * grad_primal[0] + grad_primal[1] * grad_primal[1] + grad_primal[2] * grad_primal[2])
        misfit = primal - noisy_volume
        shifted = noisy_volume + spread
        gap_terms = 0.5 * misfit * misfit + tv_weight * total_var - 0.5 * noisy_volume * noisy_volume + 0.5 * shifted * shifted
        gap_list.append(jnp.sum(gap_terms) / cell_count)
        change = updated - primal
        step_list.append(jnp.sqrt(jnp.sum(change * change) / cell_count))
        extrapolated = 2.0 * updated - primal
        primal = updated
    return (primal, jnp.stack(gap_list), jnp.stack(step_list))
```

```python
import functools

import jax
import jax.numpy as jnp
from jax import lax
from jax.experimental import pallas as pl
from jax.experimental.pallas import tpu as pltpu
from jax.sharding import PartitionSpec as P

ITERS = 4
primal_step = 0.28
dual_step = 0.28

SUB = 8
LANE = 128
HALO = ITERS
VMEM = pltpu.VMEM


def vmem_call(body, shapes, count, scratch=(), flops=1 << 20, limit=None, name=None):
    whole = pl.BlockSpec(memory_space=VMEM)
    return pl.pallas_call(
        body,
        out_shape=[jax.ShapeDtypeStruct(s, jnp.float32) for s in shapes],
        in_specs=[pl.BlockSpec(memory_space=pltpu.SMEM)] + [whole] * count,
        out_specs=[whole] * len(shapes),
        scratch_shapes=list(scratch),
        compiler_params=pltpu.CompilerParams(vmem_limit_bytes=limit),
        cost_estimate=pl.CostEstimate(flops=flops, bytes_accessed=1 << 20, transcendentals=0),
        name=name,
    )


def pack_send(half, info, noisy, weight, send_n, send_w, edge_one, edge_two):
    odd = info[0] == 1
    planes, rows, _ = noisy.shape

    def edges(to, start):
        for a, ref in enumerate((noisy, weight)):
            for j in range(planes // 2):
                to[a, j, 0:HALO] = ref[2 * j, start : start + HALO]
                to[a, j, HALO:] = ref[2 * j + 1, start : start + HALO]

    @pl.when(odd)
    def _():
        send_n[...] = noisy[:, 0 : half + SUB]
        send_w[...] = weight[:, 0 : half + SUB]
        edges(edge_one, 0)
        edges(edge_two, rows - HALO)

    @pl.when(jnp.logical_not(odd))
    def _():
        send_n[...] = noisy[:, rows - half - SUB :]
        send_w[...] = weight[:, rows - half - SUB :]
        edges(edge_one, rows - HALO)
        edges(edge_two, 0)


def put_rows(odd, to, body, body_even, body_odd, edge, a):
    planes, ext, _ = to.shape
    count = ext - HALO

    def edge_rows(z):
        half = HALO * (z % 2)
        return edge[a, z // 2, half : half + HALO]

    @pl.when(odd)
    def _():
        to[:, 0:count] = body[:, body_odd : body_odd + count]
        for z in range(planes):
            to[z, count:] = edge_rows(z)

    @pl.when(jnp.logical_not(odd))
    def _():
        to[:, HALO:] = body[:, body_even : body_even + count]
        for z in range(planes):
            to[z, 0:HALO] = edge_rows(z)


def pack_own(half, info, noisy, weight, edge, out_n, out_w):
    odd = info[0] == 1
    for a, (ref, to) in enumerate(((noisy, out_n), (weight, out_w))):
        put_rows(odd, to, ref, 0, half - HALO, edge, a)


def pack_partner(a, info, got, edge, out):
    put_rows(info[0] == 1, out, got, 0, SUB - HALO, edge, a)


def iterate(info, *refs):
    (own_n, own_w, par_n, par_w, one_n, one_w, two_n, two_w) = refs[:8]
    keep, send, stats = refs[8:11]
    noisy, weight, u, bar, p_z, p_x, p_y, cx_ref, acc = refs[11:]
    odd = info[0] == 1
    first_plane, first_row, all_planes, all_rows = info[1], info[2], info[3], info[4]
    planes, ext, cols = own_n.shape
    total = 4 * planes
    strips = ext // SUB
    chunks = cols // LANE
    half = ext - 2 * HALO

    lane = lax.broadcasted_iota(jnp.int32, (SUB, LANE), 1)
    sub = lax.broadcasted_iota(jnp.int32, (SUB, LANE), 0)
    first_sub, last_sub = sub == 0, sub == SUB - 1
    first_lane, last_lane = lane == 0, lane == LANE - 1

    for s in range(strips):
        row = first_row + s * SUB + sub
        inside = jnp.logical_and(row >= 0, row < all_rows - 1)
        cx_ref[s * SUB : (s + 1) * SUB] = jnp.where(inside, dual_step, 0.0).astype(jnp.float32)

    row_block = first_row + lax.broadcasted_iota(jnp.int32, (ext, cols), 0)
    row_in = jnp.logical_and(row_block >= 0, row_block < all_rows)

    def place(base, n_ref, w_ref):
        def one(z, _):
            value = n_ref[z]
            noisy[base + z] = value
            u[base + z] = value
            bar[base + z] = value
            plane = first_plane + base + z
            plane_in = jnp.logical_and(plane >= 0, plane < all_planes)
            weight[base + z] = jnp.where(jnp.logical_and(row_in, plane_in), w_ref[z], 1.0)
            zero = jnp.zeros_like(value)
            p_z[base + z] = zero
            p_x[base + z] = zero
            p_y[base + z] = zero
            return 0

        lax.fori_loop(0, planes, one, 0)

    @pl.when(odd)
    def _():
        place(0, one_n, one_w)
        place(planes, par_n, par_w)
        place(2 * planes, own_n, own_w)
        place(3 * planes, two_n, two_w)

    @pl.when(jnp.logical_not(odd))
    def _():
        place(0, two_n, two_w)
        place(planes, own_n, own_w)
        place(2 * planes, par_n, par_w)
        place(3 * planes, one_n, one_w)

    acc[...] = jnp.zeros_like(acc)

    def load(ref, i, s):
        return [ref[i, s * SUB : (s + 1) * SUB, c * LANE : (c + 1) * LANE] for c in range(chunks)]

    def save(ref, i, s, values):
        for c in range(chunks):
            ref[i, s * SUB : (s + 1) * SUB, c * LANE : (c + 1) * LANE] = values[c]

    def next_col(x):
        rolled = [pltpu.roll(v, LANE - 1, 1) for v in x]
        return [
            jnp.where(last_lane, rolled[c + 1], rolled[c]) if c + 1 < chunks else rolled[c]
            for c in range(chunks)
        ]

    def gradient(x, above, rolled, rolled_next, cz, cx):
        y_next = next_col(x)
        out = []
        for c in range(chunks):
            d_z = (above[c] - x[c]) * cz
            down = jnp.where(last_sub, rolled_next[c], rolled[c])
            d_x = (down - x[c]) * cx
            d_y = (y_next[c] - x[c]) * dual_step
            if c + 1 == chunks:
                d_y = jnp.where(last_lane, 0.0, d_y)
            out.append((d_z, d_x, d_y))
        return out

    def row_up(x):
        return [pltpu.roll(v, SUB - 1, 0) for v in x]

    def row_down(x):
        return [pltpu.roll(v, 1, 0) for v in x]

    def plane_step(k, i, do_u, own):
        plane = first_plane + i
        z_in = jnp.logical_and(plane >= 0, plane < all_planes - 1)
        cz = jnp.where(z_in, dual_step, 0.0).astype(jnp.float32)
        zero = jnp.zeros((SUB, LANE), jnp.float32)
        tv_sum, quad_sum, step_sum = zero, zero, zero
        bar_now = load(bar, i, 0)
        bar_roll = row_up(bar_now)
        if own:
            u_now = load(u, i, 0)
            u_roll = row_up(u_now)
        px_roll_before = None
        for s in range(strips):
            cx = cx_ref[s * SUB : (s + 1) * SUB]
            more = s + 1 < strips
            bar_next = load(bar, i, s + 1) if more else bar_now
            bar_roll_next = row_up(bar_next) if more else bar_roll
            g_bar = gradient(bar_now, load(bar, i + 1, s), bar_roll, bar_roll_next, cz, cx)
            w = load(weight, i, s)
            if own:
                u_next = load(u, i, s + 1) if more else u_now
                u_roll_next = row_up(u_next) if more else u_roll
                g_u = gradient(u_now, load(u, i + 1, s), u_roll, u_roll_next, cz, cx)
                part = zero
                for c in range(chunks):
                    a, b, d = g_u[c]
                    part = part + w[c] * jnp.sqrt(a * a + b * b + d * d)
            pz, px, py = load(p_z, i, s), load(p_x, i, s), load(p_y, i, s)
            for c in range(chunks):
                a, b, d = (q + g for q, g in zip((pz[c], px[c], py[c]), g_bar[c]))
                shrink = jnp.minimum(1.0, w[c] * lax.rsqrt(a * a + b * b + d * d))
                pz[c], px[c], py[c] = a * shrink, b * shrink, d * shrink
            save(p_z, i, s, pz)
            save(p_x, i, s, px)
            save(p_y, i, s, py)
            if do_u:
                pz_below = load(p_z, i - 1, s)
                px_roll = row_down(px)
                before = px_roll_before if s else px_roll
                py_roll = [pltpu.roll(v, 1, 1) for v in py]
                n = load(noisy, i, s)
                old = u_now if own else load(u, i, s)
                new, new_bar = [], []
                quad, step = zero, zero
                for c in range(chunks):
                    x_before = jnp.where(first_sub, before[c], px_roll[c])
                    y_before = jnp.where(first_lane, py_roll[c - 1] if c else 0.0, py_roll[c])
                    spread = (pz[c] - pz_below[c]) + (px[c] - x_before) + (py[c] - y_before)
                    shifted = n[c] + spread
                    updated = (old[c] + primal_step * shifted) * (1.0 / (1.0 + primal_step))
                    change = updated - old[c]
                    new.append(updated)
                    new_bar.append(updated + change)
                    if own:
                        quad = quad + (old[c] * (0.5 * old[c] - n[c]) + 0.5 * (shifted * shifted))
                        step = step + change * change
                save(u, i, s, new)
                save(bar, i, s, new_bar)
                px_roll_before = px_roll
            if own:
                if s == 0:
                    part, quad, step = (jnp.where(sub >= HALO, v, 0.0) for v in (part, quad, step))
                if s + 1 == strips:
                    part, quad, step = (jnp.where(sub < HALO, v, 0.0) for v in (part, quad, step))
                tv_sum, quad_sum, step_sum = tv_sum + part, quad_sum + quad, step_sum + step
                u_now, u_roll = u_next, u_roll_next
            bar_now, bar_roll = bar_next, bar_roll_next
        if own:
            acc[0, k] += tv_sum
            acc[1, k] += quad_sum
            acc[2, k] += step_sum

    def sweep(k, _):
        plane_step(k, k, False, False)

        def ghost(i, _):
            plane_step(k, i, True, False)
            return 0

        def own(i, _):
            plane_step(k, i, True, True)
            return 0

        lax.fori_loop(k + 1, planes, ghost, 0)
        lax.fori_loop(planes, 3 * planes, own, 0)
        lax.fori_loop(3 * planes, total - 1 - k, ghost, 0)
        return 0

    lax.fori_loop(0, ITERS, sweep, 0)

    @pl.when(odd)
    def _():
        keep[...] = u[2 * planes : 3 * planes, HALO : HALO + half]
        send[...] = u[planes : 2 * planes, HALO : HALO + half]

    @pl.when(jnp.logical_not(odd))
    def _():
        keep[...] = u[planes : 2 * planes, HALO : HALO + half]
        send[...] = u[2 * planes : 3 * planes, HALO : HALO + half]

    for k in range(ITERS):
        gap = acc[0, k] * (1.0 / dual_step) + acc[1, k]
        stats[k : k + 1] = jnp.sum(gap, axis=0, keepdims=True)
        stats[ITERS + k : ITERS + k + 1] = jnp.sum(acc[2, k], axis=0, keepdims=True)


def pack_out(info, keep, got, out):
    odd = info[0] == 1
    half = keep.shape[1]

    @pl.when(odd)
    def _():
        out[:, 0:half] = got[...]
        out[:, half:] = keep[...]

    @pl.when(jnp.logical_not(odd))
    def _():
        out[:, 0:half] = keep[...]
        out[:, half:] = got[...]


def shards(noisy_volume, tv_weight):
    planes, rows, cols = noisy_volume.shape
    count_z, count_x = lax.axis_size("gz"), lax.axis_size("gx")
    if planes < ITERS or planes % 2 or count_z % 2 or rows % (2 * SUB) or cols % LANE:
        raise ValueError("unsupported sizes")
    half = rows // 2
    ext = half + 2 * HALO
    cell_count = planes * rows * cols * count_z * count_x
    both = ("gz", "gx")
    gz, gx = lax.axis_index("gz"), lax.axis_index("gx")
    odd = gz % 2
    pair = gz // 2
    info = jnp.stack(
        [
            odd,
            (2 * pair - 1) * planes,
            gx * rows + odd * half - HALO,
            jnp.int32(planes * count_z),
            jnp.int32(rows * count_x),
        ]
    ).astype(jnp.int32)

    def permute(value, step):
        pairs = []
        for z in range(count_z):
            for x in range(count_x):
                tz, tx = step(z, x)
                if 0 <= tz < count_z and 0 <= tx < count_x:
                    pairs.append((z * count_x + x, tz * count_x + tx))
        return lax.ppermute(value, both, pairs)

    swap = lambda z, x: (z ^ 1, x)
    edge_step_one = lambda z, x: (z, x - 1 if z % 2 else x + 1)
    edge_step_two = lambda z, x: (z ^ 1, x + 1 if z % 2 else x - 1)
    ghost_step_one = lambda z, x: (z + 2 if z % 2 else z - 2, x)
    ghost_step_two = lambda z, x: (z - 2 if z % 2 else z + 2, x)

    block = (planes, ext, cols)
    edge = (2, planes // 2, 2 * HALO, cols)
    send_shape = (planes, half + SUB, cols)
    send_n, send_w, edge_one, edge_two = vmem_call(
        functools.partial(pack_send, half), [send_shape] * 2 + [edge] * 2, 2, name="pack_send"
    )(info, noisy_volume, tv_weight)
    got_n = permute(send_n, swap)
    got_one = permute(edge_one, edge_step_one)
    got_two = permute(edge_two, edge_step_two)
    got_w = permute(send_w, swap)
    own_n, own_w = vmem_call(functools.partial(pack_own, half), [block] * 2, 3, name="pack_own")(
        info, noisy_volume, tv_weight, got_one
    )
    one_n = permute(own_n, ghost_step_one)
    one_w = permute(own_w, ghost_step_one)
    (par_n,) = vmem_call(functools.partial(pack_partner, 0), [block], 2, name="pack_partner")(
        info, got_n, got_two
    )
    two_n = permute(par_n, ghost_step_two)
    (par_w,) = vmem_call(functools.partial(pack_partner, 1), [block], 2, name="pack_partner")(
        info, got_w, got_two
    )
    two_w = permute(par_w, ghost_step_two)

    out_half = (planes, half, cols)
    volume = VMEM((4 * planes, ext, cols), jnp.float32)
    keep, send, stats = vmem_call(
        iterate,
        [out_half, out_half, (2 * ITERS, LANE)],
        8,
        scratch=[volume] * 7
        + [VMEM((ext, LANE), jnp.float32), VMEM((3, ITERS, SUB, LANE), jnp.float32)],
        flops=100 << 20,
        limit=40 << 20,
        name="iterate",
    )(info, own_n, own_w, par_n, par_w, one_n, one_w, two_n, two_w)
    got = permute(send, swap)

    if count_z & (count_z - 1) or count_x & (count_x - 1):
        stats = lax.psum(stats, both)
    else:
        step = 1
        while step < count_x:
            stats = stats + permute(stats, lambda z, x, d=step: (z, x ^ d))
            step *= 2
        step = 1
        while step < count_z:
            stats = stats + permute(stats, lambda z, x, d=step: (z ^ d, x))
            step *= 2
    totals = jnp.sum(stats, axis=1) / cell_count
    (out,) = vmem_call(pack_out, [(planes, rows, cols)], 2, name="pack_out")(info, keep, got)
    return (out, totals[:ITERS], jnp.sqrt(totals[ITERS:]))


def solution(mesh):
    placed = (P("gz", "gx", None), P("gz", "gx", None))
    return jax.shard_map(
        shards,
        mesh=mesh,
        in_specs=placed,
        out_specs=(P("gz", "gx", None), P(), P()),
        check_vma=False,
    )
```

```python
import functools

import jax
import jax.numpy as jnp
from jax import lax
from jax.experimental import pallas as pl
from jax.experimental.pallas import tpu as pltpu
from jax.sharding import PartitionSpec as P

ITERS = 4
primal_step = 0.28
dual_step = 0.28

SUB = 8
LANE = 128
HALO = ITERS
VMEM = pltpu.VMEM


def vmem_call(body, shapes, spaces, scratch=(), flops=1 << 20, limit=16, name=None):
    return pl.pallas_call(
        body,
        out_shape=[jax.ShapeDtypeStruct(s, jnp.float32) for s in shapes],
        in_specs=[pl.BlockSpec(memory_space=s) for s in spaces],
        out_specs=[pl.BlockSpec(memory_space=VMEM)] * len(shapes),
        scratch_shapes=list(scratch),
        compiler_params=pltpu.CompilerParams(vmem_limit_bytes=limit << 20),
        cost_estimate=pl.CostEstimate(flops=flops, bytes_accessed=1 << 20, transcendentals=0),
        name=name,
    )


def is_odd():
    return lax.rem(lax.axis_index("gz"), 2) == 1


def by_parity(odd, when_odd, when_even):
    pl.when(odd)(when_odd)
    pl.when(jnp.logical_not(odd))(when_even)


def pack_edges(noisy, weight, edge_one, edge_two, low, high, sems):
    planes, rows, _ = noisy.shape
    copies = []
    for a, ref in enumerate((noisy, weight)):
        copies.append(pltpu.make_async_copy(ref.at[:, 0:SUB], low.at[a], sems.at[2 * a]))
        copies.append(
            pltpu.make_async_copy(ref.at[:, rows - SUB : rows], high.at[a], sems.at[2 * a + 1])
        )
    for copy in copies:
        copy.start()
    for copy in copies:
        copy.wait()

    def fill(to, ref, start):
        for a in range(2):
            for j in range(planes // 2):
                to[a, j, 0:HALO] = ref[a, 2 * j, start : start + HALO]
                to[a, j, HALO:] = ref[a, 2 * j + 1, start : start + HALO]

    def when_odd():
        fill(edge_one, low, 0)
        fill(edge_two, high, SUB - HALO)

    def when_even():
        fill(edge_one, high, SUB - HALO)
        fill(edge_two, low, 0)

    by_parity(is_odd(), when_odd, when_even)


def pack_block(parts, *refs):
    count = len(parts)
    bodies, edge, outs = refs[:count], refs[count], refs[count + 1 :]

    def fill(odd):
        for (a, body_even, body_odd), body, to in zip(parts, bodies, outs):
            planes, ext, _ = to.shape
            used = ext - HALO
            start = body_odd if odd else body_even
            if odd:
                to[:, 0:used] = body[:, start : start + used]
            else:
                to[:, HALO:] = body[:, start : start + used]
            for z in range(planes):
                half = HALO * (z % 2)
                rows = edge[a, z // 2, half : half + HALO]
                if odd:
                    to[z, used:] = rows
                else:
                    to[z, 0:HALO] = rows

    by_parity(is_odd(), lambda: fill(True), lambda: fill(False))


class Sweep:
    def __init__(self, state, weight, noisy, cx_ref, acc, offset, first_plane, all_planes):
        self.u, self.bar, self.p_z, self.p_x, self.p_y = state
        self.weight, self.noisy, self.cx_ref, self.acc = weight, noisy, cx_ref, acc
        self.offset, self.first_plane, self.all_planes = offset, first_plane, all_planes
        _, self.ext, cols = weight.shape
        self.strips, self.chunks = self.ext // SUB, cols // LANE
        lane = lax.broadcasted_iota(jnp.int32, (SUB, LANE), 1)
        self.sub = lax.broadcasted_iota(jnp.int32, (SUB, LANE), 0)
        self.first_sub, self.last_sub = self.sub == 0, self.sub == SUB - 1
        self.first_lane, self.last_lane = lane == 0, lane == LANE - 1

    def load(self, ref, m, s):
        return [
            ref[m, s * SUB : (s + 1) * SUB, c * LANE : (c + 1) * LANE] for c in range(self.chunks)
        ]

    def save(self, ref, m, s, values):
        for c in range(self.chunks):
            ref[m, s * SUB : (s + 1) * SUB, c * LANE : (c + 1) * LANE] = values[c]

    def gradient(self, x, above, rolled, rolled_next, cz, cx):
        side = [pltpu.roll(v, LANE - 1, 1) for v in x]
        out = []
        for c in range(self.chunks):
            last = c + 1 == self.chunks
            y_next = side[c] if last else jnp.where(self.last_lane, side[c + 1], side[c])
            d_z = (above[c] - x[c]) * cz
            down = jnp.where(self.last_sub, rolled_next[c], rolled[c])
            d_x = (down - x[c]) * cx
            d_y = (y_next - x[c]) * dual_step
            if last:
                d_y = jnp.where(self.last_lane, 0.0, d_y)
            out.append((d_z, d_x, d_y))
        return out

    def step(self, k, i, do_p, do_u, own):
        m = i - self.offset
        plane = self.first_plane + i
        z_in = jnp.logical_and(plane >= 0, plane < self.all_planes - 1)
        cz = jnp.where(z_in, dual_step, 0.0).astype(jnp.float32)
        zero = jnp.zeros((SUB, LANE), jnp.float32)
        tv_sum, quad_sum, step_sum = zero, zero, zero
        load, save, strips, chunks = self.load, self.save, self.strips, self.chunks
        row_up = lambda x: [pltpu.roll(v, SUB - 1, 0) for v in x]
        if do_p:
            bar_now = load(self.bar, m, 0)
            bar_roll = row_up(bar_now)
            if own:
                u_now = load(self.u, m, 0)
                u_roll = row_up(u_now)
        px_roll_before = None
        for s in range(strips):
            more = s + 1 < strips
            part, quad, step = zero, zero, zero
            if do_p:
                cx = self.cx_ref[s * SUB : (s + 1) * SUB]
                bar_next = load(self.bar, m, s + 1) if more else bar_now
                bar_roll_next = row_up(bar_next) if more else bar_roll
                above = load(self.bar, m + 1, s)
                g_bar = self.gradient(bar_now, above, bar_roll, bar_roll_next, cz, cx)
                w = load(self.weight, m, s)
                if own:
                    u_next = load(self.u, m, s + 1) if more else u_now
                    u_roll_next = row_up(u_next) if more else u_roll
                    above = load(self.u, m + 1, s)
                    g_u = self.gradient(u_now, above, u_roll, u_roll_next, cz, cx)
                    for c in range(chunks):
                        a, b, d = g_u[c]
                        part = part + w[c] * jnp.sqrt(a * a + b * b + d * d)
            pz, px, py = load(self.p_z, m, s), load(self.p_x, m, s), load(self.p_y, m, s)
            if do_p:
                for c in range(chunks):
                    a, b, d = (q + g for q, g in zip((pz[c], px[c], py[c]), g_bar[c]))
                    shrink = jnp.minimum(1.0, w[c] * lax.rsqrt(a * a + b * b + d * d))
                    pz[c], px[c], py[c] = a * shrink, b * shrink, d * shrink
                save(self.p_z, m, s, pz)
                save(self.p_x, m, s, px)
                save(self.p_y, m, s, py)
            if do_u:
                pz_below = load(self.p_z, m - 1, s)
                px_roll = [pltpu.roll(v, 1, 0) for v in px]
                before = px_roll_before if s else px_roll
                py_roll = [pltpu.roll(v, 1, 1) for v in py]
                n = load(self.noisy, m, s)
                old = u_now if own and do_p else load(self.u, m, s)
                new, new_bar = [], []
                for c in range(chunks):
                    x_before = jnp.where(self.first_sub, before[c], px_roll[c])
                    y_before = jnp.where(self.first_lane, py_roll[c - 1] if c else 0.0, py_roll[c])
                    spread = (pz[c] - pz_below[c]) + (px[c] - x_before) + (py[c] - y_before)
                    shifted = n[c] + spread
                    updated = (old[c] + primal_step * shifted) * (1.0 / (1.0 + primal_step))
                    change = updated - old[c]
                    new.append(updated)
                    new_bar.append(updated + change)
                    if own:
                        quad = quad + (old[c] * (0.5 * old[c] - n[c]) + 0.5 * (shifted * shifted))
                        step = step + change * change
                save(self.u, m, s, new)
                save(self.bar, m, s, new_bar)
                px_roll_before = px_roll
            if own:
                if s == 0:
                    part, quad, step = (
                        jnp.where(self.sub >= HALO, v, 0.0) for v in (part, quad, step)
                    )
                if not more:
                    part, quad, step = (
                        jnp.where(self.sub < HALO, v, 0.0) for v in (part, quad, step)
                    )
                tv_sum, quad_sum, step_sum = tv_sum + part, quad_sum + quad, step_sum + step
            if do_p:
                bar_now, bar_roll = bar_next, bar_roll_next
                if own:
                    u_now, u_roll = u_next, u_roll_next
        if own:
            if do_p:
                self.acc[0, k] += tv_sum
            if do_u:
                self.acc[1, k] += quad_sum
                self.acc[2, k] += step_sum

    def loop(self, k, low, high, own):
        def body(i, _):
            self.step(k, i, True, True, own)
            return 0

        lax.fori_loop(low, high, body, 0)


def place_rows(cx_ref, first_row, all_rows):
    sub = lax.broadcasted_iota(jnp.int32, (SUB, LANE), 0)
    for s in range(cx_ref.shape[0] // SUB):
        row = first_row + s * SUB + sub
        inside = jnp.logical_and(row >= 0, row < all_rows - 1)
        cx_ref[s * SUB : (s + 1) * SUB] = jnp.where(inside, dual_step, 0.0).astype(jnp.float32)


def place_weight(to, m, value, plane, first_row, all_planes, all_rows):
    row = first_row + lax.broadcasted_iota(jnp.int32, value.shape, 0)
    row_in = jnp.logical_and(row >= 0, row < all_rows)
    plane_in = jnp.logical_and(plane >= 0, plane < all_planes)
    to[m] = jnp.where(jnp.logical_and(row_in, plane_in), value, 1.0)


def geometry(planes, half, count_z, count_x):
    gz, gx = lax.axis_index("gz"), lax.axis_index("gx")
    odd = lax.rem(gz, 2)
    first_plane = (gz - odd - 1) * planes
    first_row = (2 * gx + odd) * half - HALO
    return odd == 1, first_plane, first_row, planes * count_z, 2 * half * count_x


def early(counts, own_n, own_w, par_n, par_w, one_n, one_w, send, carry, stats, *scratch):
    noisy, weight, cx_ref, acc = scratch[:4]
    state = scratch[4:]
    planes, ext, cols = own_n.shape
    half = ext - 2 * HALO
    odd, first_plane, first_row, all_planes, all_rows = geometry(planes, half, *counts)
    offset = jnp.where(odd, 0, planes)
    place_rows(cx_ref, first_row, all_rows)

    def place(base, n_ref, w_ref):
        def one(z, _):
            m = base + z
            value = n_ref[z]
            noisy[m] = value
            state[0][m] = value
            state[1][m] = value
            plane = first_plane + offset + m
            place_weight(weight, m, w_ref[z], plane, first_row, all_planes, all_rows)
            for ref in state[2:]:
                ref[m] = jnp.zeros_like(value)
            return 0

        lax.fori_loop(0, planes, one, 0)

    place(planes, par_n, par_w)

    def when_odd():
        place(0, one_n, one_w)
        place(2 * planes, own_n, own_w)

    def when_even():
        place(0, own_n, own_w)
        place(2 * planes, one_n, one_w)

    by_parity(odd, when_odd, when_even)
    acc[...] = jnp.zeros_like(acc)
    sweep = Sweep(state, weight, noisy, cx_ref, acc, offset, first_plane, all_planes)

    def iteration(k, _):
        by_parity(
            odd,
            lambda: sweep.step(k, k, True, False, False),
            lambda: sweep.step(k, planes + k, True, False, True),
        )
        sweep.loop(k, k + 1, jnp.where(odd, planes, 0), False)
        sweep.loop(
            k,
            jnp.where(odd, planes, planes + 1 + k),
            jnp.where(odd, 3 * planes - 1 - k, 3 * planes),
            True,
        )
        sweep.loop(k, 3 * planes, jnp.where(odd, 0, 4 * planes - 1 - k), False)
        return 0

    lax.fori_loop(0, ITERS, iteration, 0)
    rows = slice(HALO, HALO + half)

    def finish(first_carry, first_send):
        for a, ref in enumerate(state):
            carry[a] = ref[first_carry : first_carry + planes + 1]
        send[...] = state[0][first_send : first_send + planes, rows]

    by_parity(odd, lambda: finish(2 * planes - 1, planes), lambda: finish(0, planes))
    write_stats(stats, acc)


def write_stats(stats, acc, before=None):
    for k in range(ITERS):
        gap = acc[0, k] * (1.0 / dual_step) + acc[1, k]
        for row, value in ((k, gap), (ITERS + k, acc[2, k])):
            total = jnp.sum(value, axis=0, keepdims=True)
            if before is not None:
                total = total + before[row : row + 1]
            stats[row : row + 1] = total


def late(counts, own_n, own_w, two_n, two_w, carry, stats_in, keep, stats, *scratch):
    noisy, weight, cx_ref, acc = scratch[:4]
    state = scratch[4:]
    planes, ext, cols = own_n.shape
    half = ext - 2 * HALO
    odd, first_plane, first_row, all_planes, all_rows = geometry(planes, half, *counts)
    offset = jnp.where(odd, 2 * planes - 1, 0)
    place_rows(cx_ref, first_row, all_rows)

    def place(base, n_ref, w_ref, fresh):
        def one(z, _):
            m = base + z
            value = n_ref[z]
            noisy[m] = value
            plane = first_plane + offset + m
            place_weight(weight, m, w_ref[z], plane, first_row, all_planes, all_rows)
            if fresh:
                state[0][m] = value
                state[1][m] = value
                for ref in state[2:]:
                    ref[m] = jnp.zeros_like(value)
            return 0

        lax.fori_loop(0, planes, one, 0)

    def restore(base):
        def one(z, _):
            for a, ref in enumerate(state):
                ref[base + z] = carry[a, z]
            return 0

        lax.fori_loop(0, planes + 1, one, 0)

    def when_odd():
        restore(0)
        place(1, own_n, own_w, False)
        place(planes + 1, two_n, two_w, True)

    def when_even():
        place(0, two_n, two_w, True)
        place(planes, own_n, own_w, False)
        restore(planes)

    by_parity(odd, when_odd, when_even)
    acc[...] = jnp.zeros_like(acc)
    sweep = Sweep(state, weight, noisy, cx_ref, acc, offset, first_plane, all_planes)
    even = jnp.logical_not(odd)

    def iteration(k, _):
        @pl.when(even)
        def _():
            sweep.step(k, k, True, False, False)

        sweep.loop(k, k + 1, jnp.where(odd, 0, planes), False)
        sweep.loop(
            k,
            jnp.where(odd, 3 * planes - 1 - k, planes),
            jnp.where(odd, 3 * planes, planes + k),
            True,
        )
        sweep.loop(k, 3 * planes, jnp.where(odd, 4 * planes - 1 - k, 0), False)

        @pl.when(even)
        def _():
            sweep.step(k, planes + k, False, True, True)

        return 0

    lax.fori_loop(0, ITERS, iteration, 0)
    rows = slice(HALO, HALO + half)

    def finish(first):
        keep[...] = state[0][first : first + planes, rows]

    by_parity(odd, lambda: finish(1), lambda: finish(planes))
    write_stats(stats, acc, stats_in)


def pack_out(keep, got, out):
    half = keep.shape[1]

    def when_odd():
        out[:, 0:half] = got[...]
        out[:, half:] = keep[...]

    def when_even():
        out[:, 0:half] = keep[...]
        out[:, half:] = got[...]

    by_parity(is_odd(), when_odd, when_even)


def shards(noisy_volume, tv_weight):
    planes, rows, cols = noisy_volume.shape
    count_z, count_x = lax.axis_size("gz"), lax.axis_size("gx")
    if planes != ITERS or count_z % 2 or rows % (2 * SUB) or cols % LANE:
        raise ValueError("unsupported sizes")
    half = rows // 2
    ext = half + 2 * HALO
    cell_count = planes * rows * cols * count_z * count_x
    both = ("gz", "gx")
    odd = lax.rem(lax.axis_index("gz"), 2)

    def permute(value, step):
        pairs = []
        for z in range(count_z):
            for x in range(count_x):
                tz, tx = step(z, x)
                if 0 <= tz < count_z and 0 <= tx < count_x:
                    pairs.append((z * count_x + x, tz * count_x + tx))
        return lax.ppermute(value, both, pairs)

    swap = lambda z, x: (z ^ 1, x)
    edge_step_one = lambda z, x: (z, x - 1 if z % 2 else x + 1)
    edge_step_two = lambda z, x: (z ^ 1, x + 1 if z % 2 else x - 1)
    ghost_step_one = lambda z, x: (z + 2 if z % 2 else z - 2, x)
    ghost_step_two = lambda z, x: (z - 2 if z % 2 else z + 2, x)

    block = (planes, ext, cols)
    edge = (2, planes // 2, 2 * HALO, cols)
    near = (2, planes, SUB, cols)
    sent = (planes, half + SUB, cols)
    start = (1 - odd) * (rows - half - SUB)
    zero = jnp.zeros_like(start)
    send_n = lax.dynamic_slice(noisy_volume, (zero, start, zero), sent)
    got_n = permute(send_n, swap)
    edge_one, edge_two = vmem_call(
        pack_edges,
        [edge] * 2,
        [pl.ANY] * 2,
        scratch=[VMEM(near, jnp.float32)] * 2 + [pltpu.SemaphoreType.DMA((4,))],
        name="pack_edges",
    )(noisy_volume, tv_weight)
    got_one = permute(edge_one, edge_step_one)
    got_two = permute(edge_two, edge_step_two)
    send_w = lax.dynamic_slice(tv_weight, (zero, start, zero), sent)
    got_w = permute(send_w, swap)

    def pack(parts, bodies, got_edge, name):
        return vmem_call(
            functools.partial(pack_block, parts),
            [block] * len(parts),
            [VMEM] * (len(parts) + 1),
            name=name,
        )(*bodies, got_edge)

    own_n, own_w = pack(
        [(0, 0, half - HALO), (1, 0, half - HALO)], [noisy_volume, tv_weight], got_one, "pack_own"
    )
    one_n = permute(own_n, ghost_step_one)
    one_w = permute(own_w, ghost_step_one)
    (par_n,) = pack([(0, 0, SUB - HALO)], [got_n], got_two, "pack_partner_n")
    two_n = permute(par_n, ghost_step_two)
    (par_w,) = pack([(1, 0, SUB - HALO)], [got_w], got_two, "pack_partner_w")
    two_w = permute(par_w, ghost_step_two)

    out_half = (planes, half, cols)
    stats_shape = (2 * ITERS, LANE)
    counts = (count_z, count_x)
    small = [VMEM((ext, LANE), jnp.float32), VMEM((3, ITERS, SUB, LANE), jnp.float32)]

    def volumes(depth):
        one = VMEM((depth, ext, cols), jnp.float32)
        return [one] * 2 + small + [one] * 5

    send, carry, stats_early = vmem_call(
        functools.partial(early, counts),
        [out_half, (5, planes + 1, ext, cols), stats_shape],
        [VMEM] * 6,
        scratch=volumes(3 * planes),
        flops=100 << 20,
        limit=32,
        name="early",
    )(own_n, own_w, par_n, par_w, one_n, one_w)
    got = permute(send, swap)
    keep, stats = vmem_call(
        functools.partial(late, counts),
        [out_half, stats_shape],
        [VMEM] * 6,
        scratch=volumes(2 * planes + 1),
        flops=50 << 20,
        limit=32,
        name="late",
    )(own_n, own_w, two_n, two_w, carry, stats_early)

    if count_z & (count_z - 1) or count_x & (count_x - 1):
        stats = lax.psum(stats, both)
    else:
        step = 1
        while step < count_x:
            stats = stats + permute(stats, lambda z, x, d=step: (z, x ^ d))
            step *= 2
        step = 1
        while step < count_z:
            stats = stats + permute(stats, lambda z, x, d=step: (z ^ d, x))
            step *= 2
    totals = jnp.sum(stats, axis=1) / cell_count
    (out,) = vmem_call(pack_out, [(planes, rows, cols)], [VMEM] * 2, name="pack_out")(keep, got)
    return (out, totals[:ITERS], jnp.sqrt(totals[ITERS:]))


def solution(mesh):
    placed = (P("gz", "gx", None), P("gz", "gx", None))
    return jax.shard_map(
        shards,
        mesh=mesh,
        in_specs=placed,
        out_specs=(P("gz", "gx", None), P(), P()),
        check_vma=False,
    )
```

```python
import functools

import jax
import jax.numpy as jnp
from jax import lax
from jax.experimental import pallas as pl
from jax.experimental.pallas import tpu as pltpu
from jax.sharding import PartitionSpec as P


ITERS = 4
primal_step = 0.28
dual_step = 0.28

SUB = 8
LANE = 128
HALO = ITERS
VMEM = pltpu.VMEM


def vmem_call(body, shapes, spaces, scratch=(), flops=1 << 20, limit=16, aliases=None):
    return pl.pallas_call(
        body,
        out_shape=[jax.ShapeDtypeStruct(s, jnp.float32) for s in shapes],
        in_specs=[pl.BlockSpec(memory_space=s) for s in spaces],
        out_specs=[pl.BlockSpec(memory_space=VMEM)] * len(shapes),
        scratch_shapes=list(scratch),
        input_output_aliases=aliases or {},
        compiler_params=pltpu.CompilerParams(vmem_limit_bytes=limit << 20),
        cost_estimate=pl.CostEstimate(flops=flops, bytes_accessed=1 << 20, transcendentals=0),
    )


def is_odd():
    return lax.rem(lax.axis_index("gz"), 2) == 1


def by_parity(odd, when_odd, when_even):
    pl.when(odd)(when_odd)
    pl.when(jnp.logical_not(odd))(when_even)


def move_rows(planes, rows, half, odd, whole, send, own):
    used = half + HALO
    for z in range(planes):
        base = used * (z % 2)
        low, high = whole[z, 0:used], whole[z, rows - used : rows]
        send[z // 2][z // 2 if len(set(map(id, send))) == 1 else 0, base : base + used] = (
            low if odd else high
        )
        own[z // 2, base : base + used] = high if odd else low


def pack_first(noisy, weight, send_n, own_n, edge_one, edge_two, whole, low, high, sems):
    planes, rows, _ = noisy.shape
    half = rows // 2
    copies = [
        pltpu.make_async_copy(noisy, whole, sems.at[0]),
        pltpu.make_async_copy(weight.at[:, 0:SUB], low, sems.at[1]),
        pltpu.make_async_copy(weight.at[:, rows - SUB : rows], high, sems.at[2]),
    ]
    for copy in copies:
        copy.start()
    for copy in copies:
        copy.wait()

    def fill(to, at_low):
        for j in range(planes // 2):
            for b in range(2):
                rows_to = slice(HALO * b, HALO * (b + 1))
                z = 2 * j + b
                to[0, j, rows_to] = whole[z, 0:HALO] if at_low else whole[z, rows - HALO : rows]
                to[1, j, rows_to] = low[z, 0:HALO] if at_low else high[z, SUB - HALO : SUB]

    def run(odd):
        fill(edge_one, odd)
        fill(edge_two, not odd)
        move_rows(planes, rows, half, odd, whole, [send_n] * (planes // 2), own_n)

    by_parity(is_odd(), lambda: run(True), lambda: run(False))


def pack_second(weight, *refs):
    send, own_w, whole, sem = refs[:-3], refs[-3], refs[-2], refs[-1]
    planes, rows, _ = weight.shape
    copy = pltpu.make_async_copy(weight, whole, sem)
    copy.start()
    copy.wait()
    run = lambda odd: move_rows(planes, rows, rows // 2, odd, whole, send, own_w)
    by_parity(is_odd(), lambda: run(True), lambda: run(False))


class Sweep:
    def __init__(self, state, cx_ref, acc, first_plane, all_planes):
        self.noisy, self.weight, self.u, self.bar, self.p_z, self.p_x, self.p_y = state
        self.cx_ref, self.acc = cx_ref, acc
        self.first_plane, self.all_planes = first_plane, all_planes
        _, self.ext, cols = self.weight.shape
        self.strips, self.chunks = self.ext // SUB, cols // LANE
        lane = lax.broadcasted_iota(jnp.int32, (SUB, LANE), 1)
        self.sub = lax.broadcasted_iota(jnp.int32, (SUB, LANE), 0)
        self.first_sub, self.last_sub = self.sub == 0, self.sub == SUB - 1
        self.first_lane, self.last_lane = lane == 0, lane == LANE - 1

    def load(self, ref, m, s):
        return [
            ref[m, s * SUB : (s + 1) * SUB, c * LANE : (c + 1) * LANE] for c in range(self.chunks)
        ]

    def save(self, ref, m, s, values):
        for c in range(self.chunks):
            ref[m, s * SUB : (s + 1) * SUB, c * LANE : (c + 1) * LANE] = values[c]

    def gradient(self, x, above, rolled, rolled_next, cz, cx):
        side = [pltpu.roll(v, LANE - 1, 1) for v in x]
        out = []
        for c in range(self.chunks):
            last = c + 1 == self.chunks
            y_next = side[c] if last else jnp.where(self.last_lane, side[c + 1], side[c])
            d_z = (above[c] - x[c]) * cz
            down = jnp.where(self.last_sub, rolled_next[c], rolled[c])
            d_x = (down - x[c]) * cx
            d_y = (y_next - x[c]) * dual_step
            if last:
                d_y = jnp.where(self.last_lane, 0.0, d_y)
            out.append((d_z, d_x, d_y))
        return out

    def step(self, k, m, do_p, do_u, own, first):
        u_ref, bar_ref = (self.noisy, self.noisy) if first else (self.u, self.bar)
        plane = self.first_plane + m
        z_in = jnp.logical_and(plane >= 0, plane < self.all_planes - 1)
        cz = jnp.where(z_in, dual_step, 0.0).astype(jnp.float32)
        zero = jnp.zeros((SUB, LANE), jnp.float32)
        tv_sum, quad_sum, step_sum = zero, zero, zero
        load, save, strips, chunks = self.load, self.save, self.strips, self.chunks
        row_up = lambda x: [pltpu.roll(v, SUB - 1, 0) for v in x]
        if do_p:
            bar_now = load(bar_ref, m, 0)
            bar_roll = row_up(bar_now)
            if own and not first:
                u_now = load(u_ref, m, 0)
                u_roll = row_up(u_now)
        px_roll_before = None
        for s in range(strips):
            more = s + 1 < strips
            part, quad, step = zero, zero, zero
            if do_p:
                cx = self.cx_ref[s * SUB : (s + 1) * SUB]
                bar_next = load(bar_ref, m, s + 1) if more else bar_now
                bar_roll_next = row_up(bar_next) if more else bar_roll
                above = load(bar_ref, m + 1, s)
                g_bar = self.gradient(bar_now, above, bar_roll, bar_roll_next, cz, cx)
                w = load(self.weight, m, s)
                g_u = g_bar
                if own and not first:
                    u_next = load(u_ref, m, s + 1) if more else u_now
                    u_roll_next = row_up(u_next) if more else u_roll
                    above = load(u_ref, m + 1, s)
                    g_u = self.gradient(u_now, above, u_roll, u_roll_next, cz, cx)
                if own:
                    for c in range(chunks):
                        a, b, d = g_u[c]
                        part = part + w[c] * jnp.sqrt(a * a + b * b + d * d)
            if first and do_p:
                pz, px, py = ([None] * chunks for _ in range(3))
            else:
                pz, px, py = load(self.p_z, m, s), load(self.p_x, m, s), load(self.p_y, m, s)
            if do_p:
                for c in range(chunks):
                    a, b, d = g_bar[c]
                    if not first:
                        a, b, d = pz[c] + a, px[c] + b, py[c] + d
                    shrink = jnp.minimum(1.0, w[c] * lax.rsqrt(a * a + b * b + d * d))
                    pz[c], px[c], py[c] = a * shrink, b * shrink, d * shrink
                save(self.p_z, m, s, pz)
                save(self.p_x, m, s, px)
                save(self.p_y, m, s, py)
            if do_u:
                pz_below = load(self.p_z, m - 1, s)
                px_roll = [pltpu.roll(v, 1, 0) for v in px]
                before = px_roll_before if s else px_roll
                py_roll = [pltpu.roll(v, 1, 1) for v in py]
                n = load(self.noisy, m, s)
                old = u_now if own and do_p and not first else load(u_ref, m, s)
                new, new_bar = [], []
                for c in range(chunks):
                    x_before = jnp.where(self.first_sub, before[c], px_roll[c])
                    y_before = jnp.where(self.first_lane, py_roll[c - 1] if c else 0.0, py_roll[c])
                    spread = (pz[c] - pz_below[c]) + (px[c] - x_before) + (py[c] - y_before)
                    shifted = n[c] + spread
                    updated = (old[c] + primal_step * shifted) * (1.0 / (1.0 + primal_step))
                    change = updated - old[c]
                    new.append(updated)
                    new_bar.append(updated + change)
                    if own:
                        quad = quad + (old[c] * (0.5 * old[c] - n[c]) + 0.5 * (shifted * shifted))
                        step = step + change * change
                save(self.u, m, s, new)
                save(self.bar, m, s, new_bar)
                px_roll_before = px_roll
            if own:
                if s == 0:
                    part, quad, step = (
                        jnp.where(self.sub >= HALO, v, 0.0) for v in (part, quad, step)
                    )
                if not more:
                    part, quad, step = (
                        jnp.where(self.sub < HALO, v, 0.0) for v in (part, quad, step)
                    )
                tv_sum, quad_sum, step_sum = tv_sum + part, quad_sum + quad, step_sum + step
            if do_p:
                bar_now, bar_roll = bar_next, bar_roll_next
                if own and not first:
                    u_now, u_roll = u_next, u_roll_next
        if own:
            if do_p:
                self.acc[0, k] += tv_sum
            if do_u:
                self.acc[1, k] += quad_sum
                self.acc[2, k] += step_sum

    def loop(self, k, low, high, own, first):
        def body(i, _):
            self.step(k, i, True, True, own, first)
            return 0

        lax.fori_loop(low, high, body, 0)


def place_rows(cx_ref, first_row, all_rows):
    sub = lax.broadcasted_iota(jnp.int32, (SUB, LANE), 0)
    for s in range(cx_ref.shape[0] // SUB):
        row = first_row + s * SUB + sub
        inside = jnp.logical_and(row >= 0, row < all_rows - 1)
        cx_ref[s * SUB : (s + 1) * SUB] = jnp.where(inside, dual_step, 0.0).astype(jnp.float32)


def place(odd, base, raw_n, raw_w, edge, state, edge_in, block_in):
    noisy, weight = state[:2]
    planes = 2 * edge.shape[1]
    ext = noisy.shape[1]
    used = ext - HALO
    body = slice(0, used) if odd else slice(HALO, ext)
    rim = slice(used, ext) if odd else slice(0, HALO)
    for z in range(planes):
        j, b = z // 2, z % 2
        rows, edge_rows = slice(used * b, used * (b + 1)), slice(HALO * b, HALO * (b + 1))
        value = raw_w[j][rows]
        if block_in is not None:
            value = jnp.where(block_in, value, 1.0)
            in_rim = jnp.logical_and(edge_in, block_in)
        else:
            in_rim = edge_in
        noisy[base + z, body] = raw_n[j][rows]
        noisy[base + z, rim] = edge[0, j, edge_rows]
        weight[base + z, body] = value
        weight[base + z, rim] = jnp.where(in_rim, edge[1, j, edge_rows], 1.0)


def geometry(planes, half, count_z, count_x):
    gz, gx = lax.axis_index("gz"), lax.axis_index("gx")
    odd = lax.rem(gz, 2)
    first_plane = (gz - odd - 1) * planes
    first_row = (2 * gx + odd) * half - HALO
    below, above = gz >= 2, gz < count_z - 2
    edge_in = (gx < count_x - 1, gx > 0)
    return odd == 1, first_plane, first_row, planes * count_z, 2 * half * count_x, edge_in, below, above


def split(ref):
    return [ref.at[j] for j in range(ref.shape[0])]


def early(counts, *refs):
    own_n, own_w, par_n, par_w0, par_w1, one_n, one_w, edge_own, edge_par, edge_far = refs[:10]
    send, stats = refs[10:12]
    state, (cx_ref, acc) = refs[12:19], refs[19:]
    planes, half = send.shape[0], send.shape[1]
    odd, first_plane, first_row, all_planes, all_rows, edge_in, below, above = geometry(
        planes, half, *counts
    )
    place_rows(cx_ref, first_row, all_rows)
    par_w = [par_w0.at[0], par_w1.at[0]]

    def when_odd():
        place(True, 0, split(one_n), split(one_w), edge_far, state, edge_in[0], below)
        place(True, planes, split(par_n), par_w, edge_par, state, edge_in[0], None)
        place(True, 2 * planes, split(own_n), split(own_w), edge_own, state, edge_in[0], None)

    def when_even():
        place(False, planes, split(own_n), split(own_w), edge_own, state, edge_in[1], None)
        place(False, 2 * planes, split(par_n), par_w, edge_par, state, edge_in[1], None)
        place(False, 3 * planes, split(one_n), split(one_w), edge_far, state, edge_in[1], above)

    by_parity(odd, when_odd, when_even)
    acc[...] = jnp.zeros_like(acc)
    sweep = Sweep(state, cx_ref, acc, first_plane, all_planes)

    def iteration(k, first):
        by_parity(
            odd,
            lambda: sweep.step(k, k, True, False, False, first),
            lambda: sweep.step(k, planes + k, True, False, True, first),
        )
        sweep.loop(k, k + 1, jnp.where(odd, planes, 0), False, first)
        sweep.loop(
            k,
            jnp.where(odd, planes, planes + 1 + k),
            jnp.where(odd, 3 * planes - 1 - k, 3 * planes),
            True,
            first,
        )
        sweep.loop(k, 3 * planes, jnp.where(odd, 0, 4 * planes - 1 - k), False, first)

    iterations(iteration)

    def finish(first_send):
        send[...] = state[2][first_send : first_send + planes, HALO : HALO + half]

    by_parity(odd, lambda: finish(planes), lambda: finish(2 * planes))
    write_stats(stats, acc)


def iterations(iteration):
    iteration(0, True)

    def body(k, _):
        iteration(k, False)
        return 0

    lax.fori_loop(1, ITERS, body, 0)


def write_stats(stats, acc, before=None):
    for k in range(ITERS):
        gap = acc[0, k] * (1.0 / dual_step) + acc[1, k]
        for row, value in ((k, gap), (ITERS + k, acc[2, k])):
            total = jnp.sum(value, axis=0, keepdims=True)
            if before is not None:
                total = total + before[row : row + 1]
            stats[row : row + 1] = total


def late(counts, *refs):
    two_n, two_w0, two_w1, edge_far, stats_in = refs[:5]
    keep, stats = refs[12:14]
    state, (cx_ref, acc) = refs[14:21], refs[21:]
    planes, half = keep.shape[0], keep.shape[1]
    odd, first_plane, first_row, all_planes, all_rows, edge_in, below, above = geometry(
        planes, half, *counts
    )
    place_rows(cx_ref, first_row, all_rows)
    two_w = [two_w0.at[0], two_w1.at[0]]
    by_parity(
        odd,
        lambda: place(True, 3 * planes, split(two_n), two_w, edge_far, state, edge_in[0], above),
        lambda: place(False, 0, split(two_n), two_w, edge_far, state, edge_in[1], below),
    )
    acc[...] = jnp.zeros_like(acc)
    sweep = Sweep(state, cx_ref, acc, first_plane, all_planes)
    even = jnp.logical_not(odd)

    def iteration(k, first):
        pl.when(even)(lambda: sweep.step(k, k, True, False, False, first))
        sweep.loop(k, k + 1, jnp.where(odd, 0, planes), False, first)
        sweep.loop(
            k,
            jnp.where(odd, 3 * planes - 1 - k, planes),
            jnp.where(odd, 3 * planes, planes + k),
            True,
            first,
        )
        sweep.loop(k, 3 * planes, jnp.where(odd, 4 * planes - 1 - k, 0), False, first)
        pl.when(even)(lambda: sweep.step(k, planes + k, False, True, True, first))

    iterations(iteration)

    def finish(first):
        keep[...] = state[2][first : first + planes, HALO : HALO + half]

    by_parity(odd, lambda: finish(2 * planes), lambda: finish(planes))
    write_stats(stats, acc, stats_in)


def pack_out(keep, got, out):
    half = keep.shape[1]

    def when_odd():
        out[:, 0:half] = got[...]
        out[:, half:] = keep[...]

    def when_even():
        out[:, 0:half] = keep[...]
        out[:, half:] = got[...]

    by_parity(is_odd(), when_odd, when_even)


def shards(noisy_volume, tv_weight):
    planes, rows, cols = noisy_volume.shape
    count_z, count_x = lax.axis_size("gz"), lax.axis_size("gx")
    if planes != ITERS or count_z % 2 or rows % (2 * SUB) or cols % LANE:
        raise ValueError("unsupported sizes")
    half = rows // 2
    ext = half + 2 * HALO
    cell_count = planes * rows * cols * count_z * count_x
    both = ("gz", "gx")

    def permute(value, step):
        pairs = []
        for z in range(count_z):
            for x in range(count_x):
                tz, tx = step(z, x)
                if 0 <= tz < count_z and 0 <= tx < count_x:
                    pairs.append((z * count_x + x, tz * count_x + tx))
        return lax.ppermute(value, both, pairs)

    swap = lambda z, x: (z ^ 1, x)
    edge_step_one = lambda z, x: (z, x - 1 if z % 2 else x + 1)
    edge_step_two = lambda z, x: (z ^ 1, x + 1 if z % 2 else x - 1)
    ghost_step_one = lambda z, x: (z + 2 if z % 2 else z - 2, x)
    ghost_step_two = lambda z, x: (z - 2 if z % 2 else z + 2, x)

    edge = (2, planes // 2, 2 * HALO, cols)
    raw = (planes // 2, 2 * (half + HALO), cols)
    chunk = (1,) + raw[1:]
    near = VMEM((planes, SUB, cols), jnp.float32)
    whole = VMEM((planes, rows, cols), jnp.float32)
    send_n, own_n, edge_one, edge_two = vmem_call(
        pack_first,
        [raw, raw, edge, edge],
        [pltpu.HBM] * 2,
        scratch=[whole, near, near, pltpu.SemaphoreType.DMA((3,))],
    )(*(pltpu.with_memory_space_constraint(v, pltpu.HBM) for v in (noisy_volume, tv_weight)))
    edge_par = permute(edge_two, edge_step_two)
    par_n = permute(send_n, swap)
    one_n = permute(own_n, ghost_step_one)
    *send_w, own_w = vmem_call(
        pack_second,
        [chunk] * (planes // 2) + [raw],
        [pltpu.HBM],
        scratch=[whole, pltpu.SemaphoreType.DMA],
    )(pltpu.with_memory_space_constraint(tv_weight, pltpu.HBM))
    par_w = [permute(value, swap) for value in send_w]
    edge_own = permute(edge_one, edge_step_one)
    one_w = permute(own_w, ghost_step_one)
    edge_one_far = permute(edge_own, ghost_step_one)
    edge_two_far = permute(edge_par, ghost_step_two)
    two_n = permute(par_n, ghost_step_two)
    two_w = [permute(value, ghost_step_two) for value in par_w]

    out_half = (planes, half, cols)
    stats_shape = (2 * ITERS, LANE)
    counts = (count_z, count_x)
    small = [VMEM((ext, LANE), jnp.float32), VMEM((3, ITERS, SUB, LANE), jnp.float32)]
    states = [(4 * planes, ext, cols)] * 7
    send, stats, *state = vmem_call(
        functools.partial(early, counts),
        [out_half, stats_shape] + states,
        [VMEM] * 10,
        scratch=small,
        flops=100 << 20,
        limit=24,
    )(own_n, own_w, par_n, *par_w, one_n, one_w, edge_own, edge_par, edge_one_far)
    got = permute(send, swap)
    keep, stats, *_ = vmem_call(
        functools.partial(late, counts),
        [out_half, stats_shape] + states,
        [VMEM] * 12,
        scratch=small,
        flops=50 << 20,
        limit=24,
        aliases={5 + a: 2 + a for a in range(7)},
    )(two_n, *two_w, edge_two_far, stats, *state)

    if count_z & (count_z - 1) or count_x & (count_x - 1):
        stats = lax.psum(stats, both)
    else:
        step = 1
        while step < count_x:
            stats = stats + permute(stats, lambda z, x, d=step: (z, x ^ d))
            step *= 2
        step = 1
        while step < count_z:
            stats = stats + permute(stats, lambda z, x, d=step: (z ^ d, x))
            step *= 2
    totals = jnp.sum(stats, axis=1) / cell_count
    (out,) = vmem_call(pack_out, [(planes, rows, cols)], [VMEM] * 2)(keep, got)
    return (out, totals[:ITERS], jnp.sqrt(totals[ITERS:]))


def solution(mesh):
    placed = (P("gz", "gx", None), P("gz", "gx", None))

    return jax.shard_map(
        shards,
        mesh=mesh,
        in_specs=placed,
        out_specs=(P("gz", "gx", None), P(), P()),
        check_vma=False,
    )
```

```python
import functools

import jax
import jax.numpy as jnp
from jax import lax
from jax.experimental import pallas as pl
from jax.experimental.pallas import tpu as pltpu
from jax.sharding import PartitionSpec as P


ITERS = 4
primal_step = 0.28
dual_step = 0.28

SUB = 8
PIECES = 3
LANE = 128
HALO = ITERS
KEEP_SHARE = 1.0 / (1.0 + primal_step)
NEW_SHARE = primal_step / (1.0 + primal_step)
TINY = 2.0**-126
VMEM = pltpu.VMEM


def vmem_call(body, shapes, spaces, scratch=(), flops=1 << 20, limit=16, aliases=None):
    return pl.pallas_call(
        body,
        out_shape=[jax.ShapeDtypeStruct(s, jnp.float32) for s in shapes],
        in_specs=[pl.BlockSpec(memory_space=s) for s in spaces],
        out_specs=[pl.BlockSpec(memory_space=VMEM)] * len(shapes),
        scratch_shapes=list(scratch),
        input_output_aliases=aliases or {},
        compiler_params=pltpu.CompilerParams(vmem_limit_bytes=limit << 20),
        cost_estimate=pl.CostEstimate(flops=flops, bytes_accessed=1 << 20, transcendentals=0),
    )


def is_odd():
    return lax.rem(lax.axis_index("gz"), 2) == 1


def by_parity(odd, when_odd, when_even):
    pl.when(odd)(when_odd)
    pl.when(jnp.logical_not(odd))(when_even)


def unit_rows(sizes, used):
    return [(piece, used * j) for piece, size in enumerate(sizes) for j in range(size)]


def pack(noisy, weight, *refs):
    *send, own, edge_one, edge_two, whole, sems = refs
    planes, rows, _ = noisy.shape
    used = rows // 2 + HALO
    copies = [
        pltpu.make_async_copy(ref, whole.at[a], sems.at[a]) for a, ref in enumerate((noisy, weight))
    ]
    for copy in copies:
        copy.start()
    for copy in copies:
        copy.wait()
    places = unit_rows([ref.shape[0] // used for ref in send], used)

    def run(odd):
        for to, at_low in ((edge_one, odd), (edge_two, not odd)):
            for unit in range(2 * planes):
                a, z = unit // planes, unit % planes
                rows_to = slice(HALO * (z % 2), HALO * (z % 2 + 1))
                first = 0 if at_low else rows - HALO
                to[a, z // 2, rows_to] = whole[a, z, first : first + HALO]
        for unit, (piece, base) in enumerate(places):
            a, z = unit // planes, unit % planes
            low, high = slice(0, used), slice(rows - used, rows)
            send[piece][base : base + used] = whole[a, z, low if odd else high]
            own[used * unit : used * (unit + 1)] = whole[a, z, high if odd else low]

    by_parity(is_odd(), lambda: run(True), lambda: run(False))


class Sweep:
    def __init__(self, state, cx_ref, acc, first_plane, all_planes):
        self.noisy, self.weight, self.u, self.bar, self.p_z, self.p_x, self.p_y = state
        self.cx_ref, self.acc = cx_ref, acc
        self.first_plane, self.all_planes = first_plane, all_planes
        _, self.ext, cols = self.weight.shape
        self.strips, self.chunks = self.ext // SUB, cols // LANE
        lane = lax.broadcasted_iota(jnp.int32, (SUB, LANE), 1)
        self.sub = lax.broadcasted_iota(jnp.int32, (SUB, LANE), 0)
        self.first_sub, self.last_sub = self.sub == 0, self.sub == SUB - 1
        self.first_lane, self.last_lane = lane == 0, lane == LANE - 1

    def load(self, ref, m, s):
        return [
            ref[m, s * SUB : (s + 1) * SUB, c * LANE : (c + 1) * LANE] for c in range(self.chunks)
        ]

    def save(self, ref, m, s, values):
        for c in range(self.chunks):
            ref[m, s * SUB : (s + 1) * SUB, c * LANE : (c + 1) * LANE] = values[c]

    def gradient(self, x, above, rolled, rolled_next, mask):
        side = [pltpu.roll(v, LANE - 1, 1) for v in x]
        out = []
        for c in range(self.chunks):
            last = c + 1 == self.chunks
            y_next = side[c] if last else jnp.where(self.last_lane, side[c + 1], side[c])
            d_z = above[c] - x[c]
            d_x = jnp.where(self.last_sub, rolled_next[c], rolled[c]) - x[c]
            if mask is not None:
                d_x = d_x * mask
            d_y = y_next - x[c]
            if last:
                d_y = jnp.where(self.last_lane, 0.0, d_y)
            out.append((d_z, d_x, d_y))
        return out

    def step(self, k, m, do_p, do_u, own, first):
        u_ref, bar_ref = (self.noisy, self.noisy) if first else (self.u, self.bar)
        plane = self.first_plane + m
        z_in = jnp.logical_and(plane >= 0, plane < self.all_planes - 1)
        up = jnp.where(z_in, m + 1, m)
        zero = jnp.zeros((SUB, LANE), jnp.float32)
        tv_sum, quad_sum, step_sum = zero, zero, zero
        load, save, strips, chunks = self.load, self.save, self.strips, self.chunks
        row_up = lambda x: [pltpu.roll(v, SUB - 1, 0) for v in x]
        if do_p:
            bar_now = load(bar_ref, m, 0)
            bar_roll = row_up(bar_now)
            if own and not first:
                u_now = load(u_ref, m, 0)
                u_roll = row_up(u_now)
        px_roll_before = None
        for s in range(strips):
            more = s + 1 < strips
            part, quad, step = zero, zero, zero
            if do_p:
                edge = s == 0 or not more
                mask = self.cx_ref[0 if s == 0 else 1] if edge else None
                bar_next = load(bar_ref, m, s + 1) if more else bar_now
                bar_roll_next = row_up(bar_next) if more else bar_roll
                above = load(bar_ref, up, s)
                g_bar = self.gradient(bar_now, above, bar_roll, bar_roll_next, mask)
                w = load(self.weight, m, s)
                g_u = g_bar
                if own and not first:
                    u_next = load(u_ref, m, s + 1) if more else u_now
                    u_roll_next = row_up(u_next) if more else u_roll
                    above = load(u_ref, up, s)
                    g_u = self.gradient(u_now, above, u_roll, u_roll_next, mask)
                if own:
                    for c in range(chunks):
                        a, b, d = g_u[c]
                        square = a * a + b * b + d * d
                        part = part + w[c] * (square * lax.rsqrt(jnp.maximum(square, TINY)))
            if first and do_p:
                pz, px, py = ([None] * chunks for _ in range(3))
            else:
                pz, px, py = load(self.p_z, m, s), load(self.p_x, m, s), load(self.p_y, m, s)
            if do_p:
                for c in range(chunks):
                    a, b, d = g_bar[c]
                    if not first:
                        a, b, d = pz[c] + a, px[c] + b, py[c] + d
                    shrink = jnp.minimum(1.0, w[c] * lax.rsqrt(a * a + b * b + d * d))
                    pz[c], px[c], py[c] = a * shrink, b * shrink, d * shrink
                save(self.p_z, m, s, pz)
                save(self.p_x, m, s, px)
                save(self.p_y, m, s, py)
            if do_u:
                pz_below = load(self.p_z, m - 1, s)
                px_roll = [pltpu.roll(v, 1, 0) for v in px]
                before = px_roll_before if s else px_roll
                py_roll = [pltpu.roll(v, 1, 1) for v in py]
                n = load(self.noisy, m, s)
                old = u_now if own and do_p and not first else load(u_ref, m, s)
                new, new_bar = [], []
                for c in range(chunks):
                    x_before = jnp.where(self.first_sub, before[c], px_roll[c])
                    y_before = jnp.where(self.first_lane, py_roll[c - 1] if c else 0.0, py_roll[c])
                    spread = (pz[c] - pz_below[c]) + (px[c] - x_before) + (py[c] - y_before)
                    shifted = n[c] + dual_step * spread
                    updated = old[c] * KEEP_SHARE + shifted * NEW_SHARE
                    change = updated - old[c]
                    new.append(updated)
                    new_bar.append(updated + change)
                    if own:
                        quad = quad + (old[c] * (old[c] - (n[c] + n[c])) + shifted * shifted)
                        step = step + change * change
                save(self.u, m, s, new)
                save(self.bar, m, s, new_bar)
                px_roll_before = px_roll
            if own:
                if s == 0:
                    part, quad, step = (
                        jnp.where(self.sub >= HALO, v, 0.0) for v in (part, quad, step)
                    )
                if not more:
                    part, quad, step = (
                        jnp.where(self.sub < HALO, v, 0.0) for v in (part, quad, step)
                    )
                tv_sum, quad_sum, step_sum = tv_sum + part, quad_sum + quad, step_sum + step
            if do_p:
                bar_now, bar_roll = bar_next, bar_roll_next
                if own and not first:
                    u_now, u_roll = u_next, u_roll_next
        if own:
            if do_p:
                self.acc[0, k] += tv_sum
            if do_u:
                self.acc[1, k] += quad_sum
                self.acc[2, k] += step_sum

    def loop(self, k, low, high, own, first):
        def body(i, _):
            self.step(k, i, True, True, own, first)
            return 0

        lax.fori_loop(low, high, body, 0)


def place_rows(cx_ref, first_row, ext, all_rows):
    sub = lax.broadcasted_iota(jnp.int32, (SUB, LANE), 0)
    for a, first in enumerate((0, ext - SUB)):
        row = first_row + first + sub
        inside = jnp.logical_and(row >= 0, row < all_rows - 1)
        cx_ref[a] = jnp.where(inside, 1.0, 0.0).astype(jnp.float32)


def place(odd, base, units, edge, state, edge_in, block_in):
    noisy, weight = state[:2]
    planes = 2 * edge.shape[1]
    ext = noisy.shape[1]
    used = ext - HALO
    body = slice(0, used) if odd else slice(HALO, ext)
    rim = slice(used, ext) if odd else slice(0, HALO)
    for z in range(planes):
        j, b = z // 2, z % 2
        edge_rows = slice(HALO * b, HALO * (b + 1))
        n_ref, n_base = units[z]
        w_ref, w_base = units[planes + z]
        value = w_ref[w_base : w_base + used] * (1.0 / dual_step)
        in_rim = edge_in
        if block_in is not None:
            value = jnp.where(block_in, value, 1.0)
            in_rim = jnp.logical_and(edge_in, block_in)
        noisy[base + z, body] = n_ref[n_base : n_base + used]
        noisy[base + z, rim] = edge[0, j, edge_rows]
        weight[base + z, body] = value
        weight[base + z, rim] = jnp.where(in_rim, edge[1, j, edge_rows] * (1.0 / dual_step), 1.0)


def geometry(planes, half, count_z, count_x):
    gz, gx = lax.axis_index("gz"), lax.axis_index("gx")
    odd = lax.rem(gz, 2)
    first_plane = (gz - odd - 1) * planes
    first_row = (2 * gx + odd) * half - HALO
    below, above = gz >= 2, gz < count_z - 2
    edge_in = (gx < count_x - 1, gx > 0)
    return odd == 1, first_plane, first_row, planes * count_z, 2 * half * count_x, edge_in, below, above


def units_of(refs, used):
    return [
        (refs[piece], base)
        for piece, base in unit_rows([ref.shape[0] // used for ref in refs], used)
    ]


def early(counts, *refs):
    own, one, *par = refs[: 2 + PIECES]
    edge_own, edge_par, edge_far, send, stats = refs[2 + PIECES : 7 + PIECES]
    state, (cx_ref, acc) = refs[7 + PIECES : 14 + PIECES], refs[14 + PIECES :]
    planes, half = send.shape[0], send.shape[1]
    odd, first_plane, first_row, all_planes, all_rows, edge_in, below, above = geometry(
        planes, half, *counts
    )
    ext = half + 2 * HALO
    place_rows(cx_ref, first_row, ext, all_rows)
    own, one, par = (units_of(v, half + HALO) for v in ([own], [one], par))

    def when_odd():
        place(True, 0, one, edge_far, state, edge_in[0], below)
        place(True, planes, par, edge_par, state, edge_in[0], None)
        place(True, 2 * planes, own, edge_own, state, edge_in[0], None)

    def when_even():
        place(False, planes, own, edge_own, state, edge_in[1], None)
        place(False, 2 * planes, par, edge_par, state, edge_in[1], None)
        place(False, 3 * planes, one, edge_far, state, edge_in[1], above)

    by_parity(odd, when_odd, when_even)
    acc[...] = jnp.zeros_like(acc)
    sweep = Sweep(state, cx_ref, acc, first_plane, all_planes)

    def iteration(k, first):
        by_parity(
            odd,
            lambda: sweep.step(k, k, True, False, False, first),
            lambda: sweep.step(k, planes + k, True, False, True, first),
        )
        sweep.loop(k, k + 1, jnp.where(odd, planes, 0), False, first)
        sweep.loop(
            k,
            jnp.where(odd, planes, planes + 1 + k),
            jnp.where(odd, 3 * planes - 1 - k, 3 * planes),
            True,
            first,
        )
        sweep.loop(k, 3 * planes, jnp.where(odd, 0, 4 * planes - 1 - k), False, first)

    iterations(iteration)

    def finish(first_send):
        send[...] = state[2][first_send : first_send + planes, HALO : HALO + half]

    by_parity(odd, lambda: finish(planes), lambda: finish(2 * planes))
    write_stats(stats, acc)


def iterations(iteration):
    iteration(0, True)

    def body(k, _):
        iteration(k, False)
        return 0

    lax.fori_loop(1, ITERS, body, 0)


def write_stats(stats, acc, before=None):
    for k in range(ITERS):
        gap = acc[0, k] * dual_step + acc[1, k] * 0.5
        for row, value in ((k, gap), (ITERS + k, acc[2, k])):
            total = jnp.sum(value, axis=0, keepdims=True)
            if before is not None:
                total = total + before[row : row + 1]
            stats[row : row + 1] = total


def late(counts, *refs):
    *two, edge_far, stats_in = refs[: PIECES + 2]
    keep, stats = refs[PIECES + 9 : PIECES + 11]
    state, (cx_ref, acc) = refs[PIECES + 11 : PIECES + 18], refs[PIECES + 18 :]
    planes, half = keep.shape[0], keep.shape[1]
    odd, first_plane, first_row, all_planes, all_rows, edge_in, below, above = geometry(
        planes, half, *counts
    )
    ext = half + 2 * HALO
    place_rows(cx_ref, first_row, ext, all_rows)
    two = units_of(two, half + HALO)
    by_parity(
        odd,
        lambda: place(True, 3 * planes, two, edge_far, state, edge_in[0], above),
        lambda: place(False, 0, two, edge_far, state, edge_in[1], below),
    )
    acc[...] = jnp.zeros_like(acc)
    sweep = Sweep(state, cx_ref, acc, first_plane, all_planes)
    even = jnp.logical_not(odd)

    def iteration(k, first):
        pl.when(even)(lambda: sweep.step(k, k, True, False, False, first))
        sweep.loop(k, k + 1, jnp.where(odd, 0, planes), False, first)
        sweep.loop(
            k,
            jnp.where(odd, 3 * planes - 1 - k, planes),
            jnp.where(odd, 3 * planes, planes + k),
            True,
            first,
        )
        sweep.loop(k, 3 * planes, jnp.where(odd, 4 * planes - 1 - k, 0), False, first)
        pl.when(even)(lambda: sweep.step(k, planes + k, False, True, True, first))

    iterations(iteration)

    def finish(first):
        keep[...] = state[2][first : first + planes, HALO : HALO + half]

    by_parity(odd, lambda: finish(2 * planes), lambda: finish(planes))
    write_stats(stats, acc, stats_in)


def pack_out(keep, got, out):
    half = keep.shape[1]

    def when_odd():
        out[:, 0:half] = got[...]
        out[:, half:] = keep[...]

    def when_even():
        out[:, 0:half] = keep[...]
        out[:, half:] = got[...]

    by_parity(is_odd(), when_odd, when_even)


def shards(noisy_volume, tv_weight):
    planes, rows, cols = noisy_volume.shape
    count_z, count_x = lax.axis_size("gz"), lax.axis_size("gx")
    if planes != ITERS or count_z % 2 or rows % (2 * SUB) or cols % LANE:
        raise ValueError("unsupported sizes")
    half = rows // 2
    ext = half + 2 * HALO
    cell_count = planes * rows * cols * count_z * count_x
    both = ("gz", "gx")

    def permute(value, step):
        pairs = []
        for z in range(count_z):
            for x in range(count_x):
                tz, tx = step(z, x)
                if 0 <= tz < count_z and 0 <= tx < count_x:
                    pairs.append((z * count_x + x, tz * count_x + tx))
        return lax.ppermute(value, both, pairs)

    swap = lambda z, x: (z ^ 1, x)
    edge_step_one = lambda z, x: (z, x - 1 if z % 2 else x + 1)
    edge_step_two = lambda z, x: (z ^ 1, x + 1 if z % 2 else x - 1)
    ghost_step_one = lambda z, x: (z + 2 if z % 2 else z - 2, x)
    ghost_step_two = lambda z, x: (z - 2 if z % 2 else z + 2, x)
    edge_step_one_far = lambda z, x: ghost_step_one(*edge_step_one(z, x))
    edge_step_two_far = lambda z, x: ghost_step_two(*edge_step_two(z, x))

    edge = (2, planes // 2, 2 * HALO, cols)
    used = half + HALO
    sizes = [-(-(2 * planes - j) // PIECES) for j in range(PIECES)]
    outs = [(size * used, cols) for size in sizes] + [(2 * planes * used, cols), edge, edge]
    *send, own, edge_one, edge_two = vmem_call(
        pack,
        outs,
        [pltpu.HBM] * 2,
        scratch=[VMEM((2, planes, rows, cols), jnp.float32), pltpu.SemaphoreType.DMA((2,))],
    )(*(pltpu.with_memory_space_constraint(v, pltpu.HBM) for v in (noisy_volume, tv_weight)))
    edge_par = permute(edge_two, edge_step_two)
    par = [permute(value, swap) for value in send]
    one = permute(own, ghost_step_one)
    edge_own = permute(edge_one, edge_step_one)
    edge_one_far = permute(edge_one, edge_step_one_far)
    edge_two_far = permute(edge_two, edge_step_two_far)
    two = [permute(value, ghost_step_two) for value in par]

    out_half = (planes, half, cols)
    stats_shape = (2 * ITERS, LANE)
    counts = (count_z, count_x)
    small = [VMEM((2, SUB, LANE), jnp.float32), VMEM((3, ITERS, SUB, LANE), jnp.float32)]
    states = [(4 * planes, ext, cols)] * 7
    send, stats, *state = vmem_call(
        functools.partial(early, counts),
        [out_half, stats_shape] + states,
        [VMEM] * (5 + PIECES),
        scratch=small,
        flops=100 << 20,
        limit=24,
    )(own, one, *par, edge_own, edge_par, edge_one_far)
    got = permute(send, swap)
    keep, stats, *_ = vmem_call(
        functools.partial(late, counts),
        [out_half, stats_shape] + states,
        [VMEM] * (9 + PIECES),
        scratch=small,
        flops=50 << 20,
        limit=24,
        aliases={2 + PIECES + a: 2 + a for a in range(7)},
    )(*two, edge_two_far, stats, *state)

    if count_z & (count_z - 1) or count_x & (count_x - 1):
        stats = lax.psum(stats, both)
    else:
        step = 1
        while step < count_x:
            stats = stats + permute(stats, lambda z, x, d=step: (z, x ^ d))
            step *= 2
        step = 1
        while step < count_z:
            stats = stats + permute(stats, lambda z, x, d=step: (z ^ d, x))
            step *= 2
    totals = jnp.sum(stats, axis=1) / cell_count
    (out,) = vmem_call(pack_out, [(planes, rows, cols)], [VMEM] * 2)(keep, got)
    return (out, totals[:ITERS], jnp.sqrt(totals[ITERS:]))


def solution(mesh):
    placed = (P("gz", "gx", None), P("gz", "gx", None))

    return jax.shard_map(
        shards,
        mesh=mesh,
        in_specs=placed,
        out_specs=(P("gz", "gx", None), P(), P()),
        check_vma=False,
    )
```

```python
import functools

import jax
import jax.numpy as jnp
from jax import lax
from jax.experimental import pallas as pl
from jax.experimental.pallas import tpu as pltpu
from jax.sharding import PartitionSpec as P


ITERS = 4
primal_step = 0.28
dual_step = 0.28

SUB = 8
PIECES = 3
LANE = 128
HALO = ITERS
KEEP_SHARE = 1.0 / (1.0 + primal_step)
NEW_SHARE = primal_step / (1.0 + primal_step)
TINY = 2.0**-126
VMEM = pltpu.VMEM


def vmem_call(body, shapes, spaces, scratch=(), flops=1 << 20, limit=16, aliases=None):
    return pl.pallas_call(
        body,
        out_shape=[jax.ShapeDtypeStruct(s, jnp.float32) for s in shapes],
        in_specs=[pl.BlockSpec(memory_space=s) for s in spaces],
        out_specs=[pl.BlockSpec(memory_space=VMEM)] * len(shapes),
        scratch_shapes=list(scratch),
        input_output_aliases=aliases or {},
        compiler_params=pltpu.CompilerParams(vmem_limit_bytes=limit << 20),
        cost_estimate=pl.CostEstimate(flops=flops, bytes_accessed=1 << 20, transcendentals=0),
    )


def is_odd():
    return lax.rem(lax.axis_index("gz"), 2) == 1


def by_parity(odd, when_odd, when_even):
    pl.when(odd)(when_odd)
    pl.when(jnp.logical_not(odd))(when_even)


def unit_rows(sizes, used):
    return [(piece, used * j) for piece, size in enumerate(sizes) for j in range(size)]


def pack(noisy, weight, *refs):
    *send, own, edge_one, edge_two, whole, sems = refs
    planes, rows, _ = noisy.shape
    used = rows // 2 + HALO
    copies = [
        pltpu.make_async_copy(ref, whole.at[a], sems.at[a]) for a, ref in enumerate((noisy, weight))
    ]
    for copy in copies:
        copy.start()
    for copy in copies:
        copy.wait()
    places = unit_rows([ref.shape[0] // used for ref in send], used)

    def run(odd):
        for to, at_low in ((edge_one, odd), (edge_two, not odd)):
            for unit in range(2 * planes):
                a, z = unit // planes, unit % planes
                rows_to = slice(HALO * (z % 2), HALO * (z % 2 + 1))
                first = 0 if at_low else rows - HALO
                to[a, z // 2, rows_to] = whole[a, z, first : first + HALO]
        for unit, (piece, base) in enumerate(places):
            a, z = unit // planes, unit % planes
            low, high = slice(0, used), slice(rows - used, rows)
            send[piece][base : base + used] = whole[a, z, low if odd else high]
            own[used * unit : used * (unit + 1)] = whole[a, z, high if odd else low]

    by_parity(is_odd(), lambda: run(True), lambda: run(False))


class Sweep:
    def __init__(self, state, cx_ref, acc, first_plane, all_planes):
        self.noisy, self.weight, self.u, self.bar, self.p_z, self.p_x, self.p_y = state
        self.cx_ref, self.acc = cx_ref, acc
        self.first_plane, self.all_planes = first_plane, all_planes
        _, self.ext, cols = self.weight.shape
        self.strips, self.chunks = self.ext // SUB, cols // LANE
        lane = lax.broadcasted_iota(jnp.int32, (SUB, LANE), 1)
        self.sub = lax.broadcasted_iota(jnp.int32, (SUB, LANE), 0)
        self.first_sub, self.last_sub = self.sub == 0, self.sub == SUB - 1
        self.first_lane, self.last_lane = lane == 0, lane == LANE - 1

    def load(self, ref, m, s):
        return [
            ref[m, s * SUB : (s + 1) * SUB, c * LANE : (c + 1) * LANE] for c in range(self.chunks)
        ]

    def save(self, ref, m, s, values):
        for c in range(self.chunks):
            ref[m, s * SUB : (s + 1) * SUB, c * LANE : (c + 1) * LANE] = values[c]

    def gradient(self, x, above, rolled, rolled_next, z_mask, mask):
        side = [pltpu.roll(v, LANE - 1, 1) for v in x]
        out = []
        for c in range(self.chunks):
            last = c + 1 == self.chunks
            y_next = side[c] if last else jnp.where(self.last_lane, side[c + 1], side[c])
            d_z = (above[c] - x[c]) * z_mask
            d_x = jnp.where(self.last_sub, rolled_next[c], rolled[c]) - x[c]
            if mask is not None:
                d_x = d_x * mask
            d_y = y_next - x[c]
            if last:
                d_y = jnp.where(self.last_lane, 0.0, d_y)
            out.append((d_z, d_x, d_y))
        return out

    def step(self, k, m, do_p, do_u, own, first):
        u_ref, bar_ref = (self.noisy, self.noisy) if first else (self.u, self.bar)
        plane = self.first_plane + m
        z_in = jnp.logical_and(plane >= 0, plane < self.all_planes - 1)
        z_mask = jnp.where(z_in, 1.0, 0.0).astype(jnp.float32)
        zero = jnp.zeros((SUB, LANE), jnp.float32)
        tv_sum, quad_sum, step_sum = zero, zero, zero
        load, save, strips, chunks = self.load, self.save, self.strips, self.chunks
        row_up = lambda x: [pltpu.roll(v, SUB - 1, 0) for v in x]
        if do_p:
            bar_now = load(bar_ref, m, 0)
            bar_roll = row_up(bar_now)
            if own and not first:
                u_now = load(u_ref, m, 0)
                u_roll = row_up(u_now)
        px_roll_before = None
        for s in range(strips):
            more = s + 1 < strips
            part, quad, step = zero, zero, zero
            if do_p:
                edge = s == 0 or not more
                mask = self.cx_ref[0 if s == 0 else 1] if edge else None
                bar_next = load(bar_ref, m, s + 1) if more else bar_now
                bar_roll_next = row_up(bar_next) if more else bar_roll
                above = load(bar_ref, m + 1, s)
                g_bar = self.gradient(bar_now, above, bar_roll, bar_roll_next, z_mask, mask)
                w = load(self.weight, m, s)
                g_u = g_bar
                if own and not first:
                    u_next = load(u_ref, m, s + 1) if more else u_now
                    u_roll_next = row_up(u_next) if more else u_roll
                    above = load(u_ref, m + 1, s)
                    g_u = self.gradient(u_now, above, u_roll, u_roll_next, z_mask, mask)
                if own:
                    for c in range(chunks):
                        a, b, d = g_u[c]
                        square = a * a + b * b + d * d
                        part = part + w[c] * (square * lax.rsqrt(jnp.maximum(square, TINY)))
            if first and do_p:
                pz, px, py = ([None] * chunks for _ in range(3))
            else:
                pz, px, py = load(self.p_z, m, s), load(self.p_x, m, s), load(self.p_y, m, s)
            if do_p:
                for c in range(chunks):
                    a, b, d = g_bar[c]
                    if not first:
                        a, b, d = pz[c] + a, px[c] + b, py[c] + d
                    shrink = jnp.minimum(1.0, w[c] * lax.rsqrt(a * a + b * b + d * d))
                    pz[c], px[c], py[c] = a * shrink, b * shrink, d * shrink
                save(self.p_z, m, s, pz)
                save(self.p_x, m, s, px)
                save(self.p_y, m, s, py)
            if do_u:
                pz_below = load(self.p_z, m - 1, s)
                px_roll = [pltpu.roll(v, 1, 0) for v in px]
                before = px_roll_before if s else px_roll
                py_roll = [pltpu.roll(v, 1, 1) for v in py]
                n = load(self.noisy, m, s)
                old = u_now if own and do_p and not first else load(u_ref, m, s)
                new, new_bar = [], []
                for c in range(chunks):
                    x_before = jnp.where(self.first_sub, before[c], px_roll[c])
                    y_before = jnp.where(self.first_lane, py_roll[c - 1] if c else 0.0, py_roll[c])
                    spread = (pz[c] - pz_below[c]) + (px[c] - x_before) + (py[c] - y_before)
                    shifted = n[c] + dual_step * spread
                    updated = old[c] * KEEP_SHARE + shifted * NEW_SHARE
                    change = updated - old[c]
                    new.append(updated)
                    new_bar.append(updated + change)
                    if own:
                        quad = quad + (old[c] * (old[c] - (n[c] + n[c])) + shifted * shifted)
                        step = step + change * change
                save(self.u, m, s, new)
                save(self.bar, m, s, new_bar)
                px_roll_before = px_roll
            if own:
                if s == 0:
                    part, quad, step = (
                        jnp.where(self.sub >= HALO, v, 0.0) for v in (part, quad, step)
                    )
                if not more:
                    part, quad, step = (
                        jnp.where(self.sub < HALO, v, 0.0) for v in (part, quad, step)
                    )
                tv_sum, quad_sum, step_sum = tv_sum + part, quad_sum + quad, step_sum + step
            if do_p:
                bar_now, bar_roll = bar_next, bar_roll_next
                if own and not first:
                    u_now, u_roll = u_next, u_roll_next
        if own:
            if do_p:
                self.acc[0, k] += tv_sum
            if do_u:
                self.acc[1, k] += quad_sum
                self.acc[2, k] += step_sum

    def loop(self, k, low, high, own, first):
        def body(i, _):
            self.step(k, i, True, True, own, first)
            return 0

        lax.fori_loop(low, high, body, 0)


def place_rows(cx_ref, first_row, ext, all_rows):
    sub = lax.broadcasted_iota(jnp.int32, (SUB, LANE), 0)
    for a, first in enumerate((0, ext - SUB)):
        row = first_row + first + sub
        inside = jnp.logical_and(row >= 0, row < all_rows - 1)
        cx_ref[a] = jnp.where(inside, 1.0, 0.0).astype(jnp.float32)


def place(odd, base, units, edge, state, edge_in, block_in):
    noisy, weight = state[:2]
    planes = 2 * edge.shape[1]
    ext = noisy.shape[1]
    used = ext - HALO
    body = slice(0, used) if odd else slice(HALO, ext)
    rim = slice(used, ext) if odd else slice(0, HALO)
    for z in range(planes):
        j, b = z // 2, z % 2
        edge_rows = slice(HALO * b, HALO * (b + 1))
        n_ref, n_base = units[z]
        w_ref, w_base = units[planes + z]
        value = w_ref[w_base : w_base + used] * (1.0 / dual_step)
        in_rim = edge_in
        if block_in is not None:
            value = jnp.where(block_in, value, 1.0)
            in_rim = jnp.logical_and(edge_in, block_in)
        noisy[base + z, body] = n_ref[n_base : n_base + used]
        noisy[base + z, rim] = edge[0, j, edge_rows]
        weight[base + z, body] = value
        weight[base + z, rim] = jnp.where(in_rim, edge[1, j, edge_rows] * (1.0 / dual_step), 1.0)


def geometry(planes, half, count_z, count_x):
    gz, gx = lax.axis_index("gz"), lax.axis_index("gx")
    odd = lax.rem(gz, 2)
    first_plane = (gz - odd - 1) * planes
    first_row = (2 * gx + odd) * half - HALO
    below, above = gz >= 2, gz < count_z - 2
    edge_in = (gx < count_x - 1, gx > 0)
    return odd == 1, first_plane, first_row, planes * count_z, 2 * half * count_x, edge_in, below, above


def units_of(refs, used):
    return [
        (refs[piece], base)
        for piece, base in unit_rows([ref.shape[0] // used for ref in refs], used)
    ]


def early(counts, *refs):
    own, one, *par = refs[: 2 + PIECES]
    edge_own, edge_par, edge_far, send, stats = refs[2 + PIECES : 7 + PIECES]
    state, (cx_ref, acc) = refs[7 + PIECES : 14 + PIECES], refs[14 + PIECES :]
    planes, half = send.shape[0], send.shape[1]
    odd, first_plane, first_row, all_planes, all_rows, edge_in, below, above = geometry(
        planes, half, *counts
    )
    ext = half + 2 * HALO
    place_rows(cx_ref, first_row, ext, all_rows)
    own, one, par = (units_of(v, half + HALO) for v in ([own], [one], par))

    def when_odd():
        place(True, 0, one, edge_far, state, edge_in[0], below)
        place(True, planes, par, edge_par, state, edge_in[0], None)
        place(True, 2 * planes, own, edge_own, state, edge_in[0], None)

    def when_even():
        place(False, planes, own, edge_own, state, edge_in[1], None)
        place(False, 2 * planes, par, edge_par, state, edge_in[1], None)
        place(False, 3 * planes, one, edge_far, state, edge_in[1], above)

    by_parity(odd, when_odd, when_even)
    acc[...] = jnp.zeros_like(acc)
    sweep = Sweep(state, cx_ref, acc, first_plane, all_planes)

    def iteration(k, first):
        by_parity(
            odd,
            lambda: sweep.step(k, k, True, False, False, first),
            lambda: sweep.step(k, planes + k, True, False, True, first),
        )
        sweep.loop(k, k + 1, jnp.where(odd, planes, 0), False, first)
        sweep.loop(
            k,
            jnp.where(odd, planes, planes + 1 + k),
            jnp.where(odd, 3 * planes - 1 - k, 3 * planes),
            True,
            first,
        )
        sweep.loop(k, 3 * planes, jnp.where(odd, 0, 4 * planes - 1 - k), False, first)

    iterations(iteration)

    def finish(first_send):
        send[...] = state[2][first_send : first_send + planes, HALO : HALO + half]

    by_parity(odd, lambda: finish(planes), lambda: finish(2 * planes))
    write_stats(stats, acc)


def iterations(iteration):
    iteration(0, True)

    def body(k, _):
        iteration(k, False)
        return 0

    lax.fori_loop(1, ITERS, body, 0)


def write_stats(stats, acc, before=None):
    for k in range(ITERS):
        gap = acc[0, k] * dual_step + acc[1, k] * 0.5
        for row, value in ((k, gap), (ITERS + k, acc[2, k])):
            total = jnp.sum(value, axis=0, keepdims=True)
            if before is not None:
                total = total + before[row : row + 1]
            stats[row : row + 1] = total


def late(counts, *refs):
    *two, edge_far, stats_in = refs[: PIECES + 2]
    keep, stats = refs[PIECES + 9 : PIECES + 11]
    state, (cx_ref, acc) = refs[PIECES + 11 : PIECES + 18], refs[PIECES + 18 :]
    planes, half = keep.shape[0], keep.shape[1]
    odd, first_plane, first_row, all_planes, all_rows, edge_in, below, above = geometry(
        planes, half, *counts
    )
    ext = half + 2 * HALO
    place_rows(cx_ref, first_row, ext, all_rows)
    two = units_of(two, half + HALO)
    by_parity(
        odd,
        lambda: place(True, 3 * planes, two, edge_far, state, edge_in[0], above),
        lambda: place(False, 0, two, edge_far, state, edge_in[1], below),
    )
    acc[...] = jnp.zeros_like(acc)
    sweep = Sweep(state, cx_ref, acc, first_plane, all_planes)
    even = jnp.logical_not(odd)

    def iteration(k, first):
        pl.when(even)(lambda: sweep.step(k, k, True, False, False, first))
        sweep.loop(k, k + 1, jnp.where(odd, 0, planes), False, first)
        sweep.loop(
            k,
            jnp.where(odd, 3 * planes - 1 - k, planes),
            jnp.where(odd, 3 * planes, planes + k),
            True,
            first,
        )
        sweep.loop(k, 3 * planes, jnp.where(odd, 4 * planes - 1 - k, 0), False, first)
        pl.when(even)(lambda: sweep.step(k, planes + k, False, True, True, first))

    iterations(iteration)

    def finish(first):
        keep[...] = state[2][first : first + planes, HALO : HALO + half]

    by_parity(odd, lambda: finish(2 * planes), lambda: finish(planes))
    write_stats(stats, acc, stats_in)


def pack_out(keep, got, out):
    half = keep.shape[1]

    def when_odd():
        out[:, 0:half] = got[...]
        out[:, half:] = keep[...]

    def when_even():
        out[:, 0:half] = keep[...]
        out[:, half:] = got[...]

    by_parity(is_odd(), when_odd, when_even)


def shards(noisy_volume, tv_weight):
    planes, rows, cols = noisy_volume.shape
    count_z, count_x = lax.axis_size("gz"), lax.axis_size("gx")
    if planes != ITERS or count_z % 2 or rows % (2 * SUB) or cols % LANE:
        raise ValueError("unsupported sizes")
    half = rows // 2
    ext = half + 2 * HALO
    cell_count = planes * rows * cols * count_z * count_x
    both = ("gz", "gx")

    def permute(value, step):
        pairs = []
        for z in range(count_z):
            for x in range(count_x):
                tz, tx = step(z, x)
                if 0 <= tz < count_z and 0 <= tx < count_x:
                    pairs.append((z * count_x + x, tz * count_x + tx))
        return lax.ppermute(value, both, pairs)

    swap = lambda z, x: (z ^ 1, x)
    edge_step_one = lambda z, x: (z, x - 1 if z % 2 else x + 1)
    edge_step_two = lambda z, x: (z ^ 1, x + 1 if z % 2 else x - 1)
    ghost_step_one = lambda z, x: (z + 2 if z % 2 else z - 2, x)
    ghost_step_two = lambda z, x: (z - 2 if z % 2 else z + 2, x)
    edge_step_one_far = lambda z, x: ghost_step_one(*edge_step_one(z, x))
    edge_step_two_far = lambda z, x: ghost_step_two(*edge_step_two(z, x))

    edge = (2, planes // 2, 2 * HALO, cols)
    used = half + HALO
    sizes = [-(-(2 * planes - j) // PIECES) for j in range(PIECES)]
    outs = [(size * used, cols) for size in sizes] + [(2 * planes * used, cols), edge, edge]
    *send, own, edge_one, edge_two = vmem_call(
        pack,
        outs,
        [pltpu.HBM] * 2,
        scratch=[VMEM((2, planes, rows, cols), jnp.float32), pltpu.SemaphoreType.DMA((2,))],
    )(*(pltpu.with_memory_space_constraint(v, pltpu.HBM) for v in (noisy_volume, tv_weight)))
    edge_par = permute(edge_two, edge_step_two)
    par = [permute(value, swap) for value in send]
    one = permute(own, ghost_step_one)
    edge_own = permute(edge_one, edge_step_one)
    edge_one_far = permute(edge_one, edge_step_one_far)
    edge_two_far = permute(edge_two, edge_step_two_far)
    two = [permute(value, ghost_step_two) for value in par]

    out_half = (planes, half, cols)
    stats_shape = (2 * ITERS, LANE)
    counts = (count_z, count_x)
    small = [VMEM((2, SUB, LANE), jnp.float32), VMEM((3, ITERS, SUB, LANE), jnp.float32)]
    states = [(4 * planes, ext, cols)] * 7
    send, stats, *state = vmem_call(
        functools.partial(early, counts),
        [out_half, stats_shape] + states,
        [VMEM] * (5 + PIECES),
        scratch=small,
        flops=100 << 20,
        limit=24,
    )(own, one, *par, edge_own, edge_par, edge_one_far)
    got = permute(send, swap)
    keep, stats, *_ = vmem_call(
        functools.partial(late, counts),
        [out_half, stats_shape] + states,
        [VMEM] * (9 + PIECES),
        scratch=small,
        flops=50 << 20,
        limit=24,
        aliases={2 + PIECES + a: 2 + a for a in range(7)},
    )(*two, edge_two_far, stats, *state)

    if count_z & (count_z - 1) or count_x & (count_x - 1):
        stats = lax.psum(stats, both)
    else:
        step = 1
        while step < count_x:
            stats = stats + permute(stats, lambda z, x, d=step: (z, x ^ d))
            step *= 2
        step = 1
        while step < count_z:
            stats = stats + permute(stats, lambda z, x, d=step: (z ^ d, x))
            step *= 2
    totals = jnp.sum(stats, axis=1) / cell_count
    (out,) = vmem_call(pack_out, [(planes, rows, cols)], [VMEM] * 2)(keep, got)
    return (out, totals[:ITERS], jnp.sqrt(totals[ITERS:]))


def solution(mesh):
    placed = (P("gz", "gx", None), P("gz", "gx", None))

    return jax.shard_map(
        shards,
        mesh=mesh,
        in_specs=placed,
        out_specs=(P("gz", "gx", None), P(), P()),
        check_vma=False,
    )
```
